32 devices in a mesh: tm: 8 (over z, y), space: 4 (over x, core).
Axes of the slice: x: 2, y: 2, z: 4, core: 2. Of those that a mesh axis runs over, the one named last changes fastest.
Arguments:
- states: float32 [8, 3, 256, 1024], P('tm', None, 'space'), may hold values from -3 to 3
- background: float32 [3, 256, 1024], P(None, 'space'), may hold values from -3 to 3
- obs_cells: int32 [8, 4, 1024], P('tm'), may hold values from 0 to 262143
- obs_values: float32 [8, 4, 1024], P('tm'), may hold values from -3 to 3
- land_mask: int32 [256, 1024], P('space'), may hold values 0 or 1
Outputs:
- gradient: float32 [8, 3, 256, 1024], P('tm', None, 'space')
- next_states: float32 [8, 3, 256, 1024], P('tm', None, 'space')
The draws below stay inside these ranges and needn't reach their ends.
All inputs are finite; a program needn't handle non-finite values. No bound on the sum of `land_mask` on one device may be relied on, other than what follows from the above.
Results may differ from the reference program's by a relative error of at most 0.0003.
Values sent between devices are 32-bit elements; how exact they have to be, the bound alone decides.
A program may use at most 64 MiB of HBM per device.

```python
import jax
import jax.numpy as jnp
from jax import lax

NLON = 1024
NSTEP = 4
OBS = 1024
NY = 256
SUBWIN = 8


def place_ends(array, rng, least, high):
    index_at = [jax.random.randint(jax.random.fold_in(rng, axis), (), 0, length) for axis, length in enumerate(array.shape)]
    main_axis = array.shape.index(max(array.shape))
    beside = index_at[:main_axis] + [(index_at[main_axis] + 1) % array.shape[main_axis]] + index_at[main_axis + 1:]
    return array.at[tuple(index_at)].set(least).at[tuple(beside)].set(high)


def shard_levels(key, extent, shards, least, top_value):
    def one(axis_at, blocks):
        steps = jax.random.uniform(jax.random.fold_in(jax.random.fold_in(key, 6), axis_at), (blocks,), jnp.float32, least / len(shards), top_value / len(shards))
        return jnp.repeat(jnp.exp(steps), extent[axis_at] // blocks).reshape((-1,) + (1,) * (len(extent) - axis_at - 1))

    factor_of = one(*shards[0])
    for cut in shards[1:]:
        factor_of = factor_of * one(*cut)
    return factor_of


def bell_draw(own_key, shape, width, reach, split=(), dtype=jnp.bfloat16):
    gain = shard_levels(own_key, shape, split, -0.22, 0.18) if split else 1.0
    array = jax.random.normal(own_key, shape, jnp.float32) * width * gain
    return jnp.minimum(jnp.maximum(array, -reach), reach).astype(dtype)


def setup_inputs(seed: int = 0) -> dict:
    arg_keys = jax.random.split(jax.random.key(seed), 6)
    states = bell_draw(arg_keys[0], (SUBWIN, 3, NY, NLON), 0.5, 3.0, ((0, 8), (2, 4)), jnp.float32)
    background = bell_draw(arg_keys[1], (3, NY, NLON), 0.5, 3.0, ((1, 4),), jnp.float32)
    obs_cells = place_ends(jax.random.randint(arg_keys[2], (SUBWIN, NSTEP, OBS), 0, NY * NLON), jax.random.fold_in(arg_keys[2], 1), 0, (NY * NLON) - 1).astype(jnp.int32)
    obs_values = bell_draw(arg_keys[3], (SUBWIN, NSTEP, OBS), 0.5, 3.0, ((0, 8),), jnp.float32)
    land_mask = place_ends((jax.random.randint(arg_keys[4], (NY, NLON), 0, 5) < 4).astype(jnp.int32), jax.random.fold_in(arg_keys[4], 1), 0, 1)
    return dict(states=states, background=background, obs_cells=obs_cells, obs_values=obs_values, land_mask=land_mask)


advect = 0.25
gravity = 1.0
coriolis = 0.1
diffuse = 0.1
defect_weight = 2.0
obs_weight = 4.0
step_length = 0.1

def along_lon(field):
    return (jnp.roll(field, -1, axis=-1) - jnp.roll(field, 1, axis=-1)) / 2.0

def advance(padded, land):
    height, zonal, merid = (padded[0], padded[1], padded[2])
    flux_x = (1.0 + height) * zonal
    flux_y = (1.0 + height) * merid

    def laplace(field):
        inner = field[1:-1]
        return field[2:] + field[:-2] + jnp.roll(inner, 1, axis=-1) + jnp.roll(inner, -1, axis=-1) - 4.0 * inner
    diverge = along_lon(flux_x)[1:-1] + (flux_y[2:] - flux_y[:-2]) / 2.0
    h_inner, u_inner, v_inner = (height[1:-1], zonal[1:-1], merid[1:-1])
    h_new = h_inner - advect * diverge + diffuse * laplace(height)
    u_new = land * (u_inner - advect * gravity * along_lon(height)[1:-1] + coriolis * v_inner + diffuse * laplace(zonal))
    v_new = land * (v_inner - advect * gravity * (height[2:] - height[:-2]) / 2.0 - coriolis * u_inner + diffuse * laplace(merid))
    return jnp.stack([h_new, u_new, v_new])

def subwindow(state, cells, values, land):
    current = state
    misfits = []
    for step in range(NSTEP):
        current = advance(jnp.pad(current, ((0, 0), (1, 1), (0, 0))), land)
        seen = jnp.take(current[0].reshape(-1), cells[step].astype(jnp.int32))
        misfits.append(seen - values[step])
    return (current, jnp.stack(misfits))

def reference(states, background, obs_cells, obs_values, land_mask):
    land = land_mask.astype(jnp.float32)
    ends = lax.map(lambda group: subwindow(group[0], group[1], group[2], land)[0], (states, obs_cells, obs_values))
    previous = jnp.concatenate([background[None], ends[:-1]], axis=0)
    defects = states - previous
    following = jnp.concatenate([defects[1:], jnp.zeros_like(defects[:1])], axis=0)

    def adjoint(group):
        state, cells, values, ahead = group
        outputs, pullback = jax.vjp(lambda s: subwindow(s, cells, values, land), state)
        return pullback((-defect_weight * ahead, obs_weight * outputs[1]))[0]
    gradient = defect_weight * defects + lax.map(adjoint, (states, obs_cells, obs_values, following))
    updated = states - step_length * gradient
    next_states = jnp.concatenate([updated[1:], ends[-1:]], axis=0)
    return (gradient, next_states)
```

```python
import functools

import jax
import jax.numpy as jnp
from jax import lax
from jax.experimental import pallas as pl
from jax.experimental.pallas import tpu as pltpu
from jax.sharding import PartitionSpec as P

NSTEP = 4
PAD = 8
LANES = 128

advect = 0.25
gravity = 1.0
coriolis = 0.1
diffuse = 0.1
defect_weight = 2.0
obs_weight = 4.0
step_length = 0.1

KEEP = 1.0 - 4.0 * diffuse
HALF = advect / 2.0
SLOPE = HALF * (advect * gravity / 2.0)

MESH = pl.DeviceIdType.MESH


def kernel(
    n_tm,
    n_sp,
    states,
    background,
    cells_h,
    values_h,
    land,
    gradient,
    nexts,
    xr,
    yr,
    zr,
    prev_end,
    xt,
    yt,
    lam_a,
    lam_b,
    land_i,
    mask,
    dense_x,
    dense_y,
    back,
    cells,
    values,
    cells_n,
    values_n,
    load,
    send,
    recv,
):
    rows, cols = states.shape[1], states.shape[2]
    blocks = cols // LANES
    tm, sp = lax.axis_index("tm"), lax.axis_index("space")
    low, high = 2 * PAD, 2 * PAD + rows
    half_pad = PAD // 2
    has_next, has_next2 = tm < n_tm - 1, tm < n_tm - 2
    has_prev, has_prev2 = tm > 0, tm > 1
    has_up, has_down = sp > 0, sp < n_sp - 1
    every = range(blocks)

    loads = []

    def fetch(src, dst):
        entry = pltpu.make_async_copy(src, dst, load.at[len(loads)])
        entry.start()
        loads.append(entry)

    for c in every:
        part = pl.ds(c * LANES, LANES)
        fetch(states.at[:, :, part], xr.at[:, c, low:high, :])
    n_state = len(loads)
    for c in every:
        part = pl.ds(c * LANES, LANES)
        fetch(land.at[:, part], land_i.at[c, low:high, :])
    fetch(cells_h, cells)
    fetch(values_h, values)
    n_early = len(loads)
    fetch(background, back)

    for start in (0, PAD, high, high + PAD):
        blank = jnp.zeros((3, blocks, PAD, LANES), jnp.float32)
        for ref in (xr, yr, zr):
            ref[:, :, start : start + PAD, :] = blank
        land_i[:, start : start + PAD, :] = jnp.zeros((blocks, PAD, LANES), jnp.int32)

    barrier = pltpu.get_barrier_semaphore()
    near = (
        (has_up, (tm, sp - 1)),
        (has_down, (tm, sp + 1)),
        (has_prev, (tm - 1, sp)),
        (has_next, (tm + 1, sp)),
        (has_prev2, (tm - 2, sp)),
        (has_next2, (tm + 2, sp)),
    )
    for there, device in near:

        @pl.when(there)
        def _(device=device):
            pl.semaphore_signal(barrier, inc=1, device_id=device, device_id_type=MESH)

    for entry in loads[:n_early]:
        entry.wait()
    pl.semaphore_wait(barrier, sum(there.astype(jnp.int32) for there, _ in near))

    started = []

    def start(src, dst, device, sends, receives):
        index = len(started)
        entry = pltpu.make_async_remote_copy(
            src_ref=src,
            dst_ref=dst,
            send_sem=send.at[index],
            recv_sem=recv.at[index],
            device_id=device,
            device_id_type=MESH,
        )

        @pl.when(sends)
        def _():
            entry.start()

        started.append((entry, sends))
        return entry, receives

    def arrive(*pairs):
        for entry, receives in pairs:

            @pl.when(receives)
            def _(entry=entry):
                entry.wait_recv()

    def strip(ref, at):
        return ref.at[:, :, pl.ds(at, PAD), :]

    above, below = (tm, sp - 1), (tm, sp + 1)
    back1, back2, ahead = (tm - 1, sp), (tm - 2, sp), (tm + 1, sp)
    top, bottom, head, tail = PAD, high, low, high - PAD

    halo = [
        start(strip(xr, head), strip(xr, bottom), above, has_up, has_down),
        start(strip(xr, tail), strip(xr, top), below, has_down, has_up),
        start(
            land_i.at[:, pl.ds(head, PAD), :],
            land_i.at[:, pl.ds(bottom, PAD), :],
            above,
            has_up,
            has_down,
        ),
        start(
            land_i.at[:, pl.ds(tail, PAD), :],
            land_i.at[:, pl.ds(top, PAD), :],
            below,
            has_down,
            has_up,
        ),
    ]
    even = lax.rem(tm, 2) == 0
    odd = jnp.logical_not(even)
    obs_next = [
        start(cells, cells_n, back1, has_prev, has_next),
        start(values, values_n, back1, has_prev, has_next),
    ]
    pieces = [low, high - PAD, *range(low + PAD, high - PAD, PAD)]
    n_piece = len(pieces)
    far = [start(strip(xr, p), strip(zr, p), back2, has_prev2, has_next2) for p in pieces]
    direct = [start(strip(xr, p), strip(yr, p), back1, odd, even & has_next) for p in pieces]
    relayed = []

    def relay(count):
        for i in range(len(relayed), min(len(relayed) + count, n_piece)):
            arrive(far[i])
            p = pieces[i]
            relayed.append(
                start(strip(zr, p), strip(yr, p), ahead, even & has_next2, odd & has_next)
            )

    first_row = sp * rows - half_pad
    shift = cols.bit_length() - 1
    tall = rows + PAD
    wide = min(2 * LANES, cols)
    wide_shift = wide.bit_length() - 1
    level = lax.broadcasted_iota(jnp.int32, (tall, cells_h.shape[1]), 0)
    column = lax.broadcasted_iota(jnp.int32, (wide, cells_h.shape[1]), 0)

    def densify(cells, values, dense):
        def one(s, carry):
            cell = cells[pl.ds(s, 1), :]
            value = values[pl.ds(s, 1), :]
            row = lax.shift_right_logical(cell, shift) - first_row
            col = lax.bitwise_and(cell, cols - 1)
            inside = (row >= 0) & (row < tall)
            group = lax.shift_right_logical(col, wide_shift)
            key = jnp.where(inside, group * tall + row, -1)
            lane = lax.bitwise_and(col, wide - 1)
            spread = jnp.where(column == lane, 1.0, 0.0).astype(jnp.bfloat16)
            upper = value.astype(jnp.bfloat16).astype(jnp.float32)
            lower = value - upper
            for g in range(cols // wide):
                hit = level == key - g * tall
                picks = jnp.concatenate(
                    [
                        jnp.where(hit, 1.0, 0.0),
                        jnp.where(hit, upper, 0.0),
                        jnp.where(hit, lower, 0.0),
                    ],
                    axis=0,
                ).astype(jnp.bfloat16)
                out = lax.dot_general(
                    picks, spread, (((1,), (1,)), ((), ())), preferred_element_type=jnp.float32
                )
                count = obs_weight * out[:tall]
                total = count + obs_weight * (out[tall : 2 * tall] + out[2 * tall :])
                for c in range(wide // LANES):
                    at = g * (wide // LANES) + c
                    dense[s, 0, at] = count[:, c * LANES : (c + 1) * LANES]
                    dense[s, 1, at] = total[:, c * LANES : (c + 1) * LANES]
            return carry

        lax.fori_loop(0, NSTEP, one, 0)

    lane_at = lax.broadcasted_iota(jnp.int32, (PAD, LANES), 1)
    is_first, is_last = lane_at == 0, lane_at == LANES - 1

    def from_right(tiles):
        turned = [pltpu.roll(tile, LANES - 1, 1) for tile in tiles]
        return [jnp.where(is_last, turned[(c + 1) % blocks], turned[c]) for c in every]

    def from_left(tiles):
        turned = [pltpu.roll(tile, 1, 1) for tile in tiles]
        return [jnp.where(is_first, turned[c - 1], turned[c]) for c in every]

    def tile_loop(begin, count, unroll, body):
        def group(i, carry):
            for j in range(unroll):
                body(begin + (i * unroll + j) * PAD)
            return carry

        lax.fori_loop(0, count // unroll, group, 0)

    def parts(count):
        return max(u for u in (4, 3, 2, 1) if count % u == 0 and u <= 3)

    def edges(ref, fill):
        for there, at in ((has_up, top), (has_down, bottom)):

            @pl.when(jnp.logical_not(there))
            def _(at=at):
                for field in range(3):
                    value = jnp.full((blocks, PAD, LANES), fill[field], jnp.float32)
                    ref[field, :, at : at + PAD, :] = value

    def transform(raw, ref, first, last):
        def one(r):
            r = pl.multiple_of(r, PAD)
            here = pl.ds(r, PAD)
            for c in every:
                ref[0, c, here, :] = 1.0 + raw[0, c, here, :]
                ref[1, c, here, :] = HALF * raw[1, c, here, :]
                ref[2, c, here, :] = HALF * raw[2, c, here, :]

        count = (last - first) // PAD
        tile_loop(first, count, parts(count), one)

    def forward_tile(src, dst, r):
        here, up, down = pl.ds(r, PAD), pl.ds(r - 1, PAD), pl.ds(r + 1, PAD)
        q = [src[0, c, here, :] for c in every]
        u = [src[1, c, here, :] for c in every]
        v = [src[2, c, here, :] for c in every]
        slope = [SLOPE * q[c] for c in every]
        mixed = [diffuse * u[c] for c in every]
        q_right = from_right([q[c] * (diffuse - u[c]) for c in every])
        q_left = from_left([q[c] * (diffuse + u[c]) for c in every])
        u_right = from_right([mixed[c] - slope[c] for c in every])
        u_left = from_left([mixed[c] + slope[c] for c in every])
        v_right = from_right(v)
        v_left = from_left(v)
        for c in every:
            m = mask[c, here, :]
            q_up, q_down = src[0, c, up, :], src[0, c, down, :]
            v_up, v_down = src[2, c, up, :], src[2, c, down, :]
            u_sum = src[1, c, up, :] + src[1, c, down, :]
            dst[0, c, here, :] = (
                KEEP * q[c]
                + (q_right[c] + q_left[c])
                + (q_up * (diffuse + v_up) + q_down * (diffuse - v_down))
            )
            dst[1, c, here, :] = m * (
                KEEP * u[c] + coriolis * v[c] + (u_right[c] + u_left[c]) + diffuse * u_sum
            )
            dst[2, c, here, :] = m * (
                KEEP * v[c]
                - coriolis * u[c]
                + diffuse * ((v_right[c] + v_left[c]) + (v_up + v_down))
                + SLOPE * (q_up - q_down)
            )

    def forward(levels):
        full = (rows + 2 * PAD) // PAD

        def step(s, carry):
            src, dst = levels.at[s], levels.at[s + 1]
            tile_loop(top, full, parts(full), lambda r: forward_tile(src, dst, r))
            edges(dst, (1.0, 0.0, 0.0))
            return carry

        lax.fori_loop(0, NSTEP - 1, step, 0)
        src, dst = levels.at[NSTEP - 1], levels.at[NSTEP]
        count = full - 1
        tile_loop(top + half_pad, count, parts(count), lambda r: forward_tile(src, dst, r))
        edges(dst, (1.0, 0.0, 0.0))

    n_seed = (rows + PAD) // PAD
    seed_at = top + half_pad

    def drop(r):
        return pl.ds(pl.multiple_of(r - seed_at, PAD), PAD)

    def begin(levels, following, there, dense, lam):
        ends = levels.at[NSTEP]
        weight = jnp.where(there, defect_weight, 0.0)

        def one(r):
            here, at = pl.ds(r, PAD), drop(r)
            for c in every:
                m = mask[c, here, :]
                raw = [jnp.where(there, following[f, c, here, :], 0.0) for f in range(3)]
                pull = weight + dense[NSTEP - 1, 0, c, at, :]
                lam[0, c, here, :] = (
                    pull * ends[0, c, here, :]
                    - (weight + dense[NSTEP - 1, 1, c, at, :])
                    - weight * raw[0]
                )
                for f in (1, 2):
                    gap = (weight / (HALF * HALF)) * ends[f, c, here, :]
                    lam[f, c, here, :] = m * (gap - (weight / HALF) * raw[f])

        tile_loop(seed_at, n_seed, parts(n_seed), one)
        edges(lam, (0.0, 0.0, 0.0))

    def adjoint_tile(src, state, r):
        here, up, down = pl.ds(r, PAD), pl.ds(r - 1, PAD), pl.ds(r + 1, PAD)
        a = [src[0, c, here, :] for c in every]
        b = [src[1, c, here, :] for c in every]
        e = [src[2, c, here, :] for c in every]
        a_right, a_left = from_right(a), from_left(a)
        b_right, b_left = from_right(b), from_left(b)
        e_right, e_left = from_right(e), from_left(e)
        out = []
        for c in every:
            a_up, a_down = src[0, c, up, :], src[0, c, down, :]
            e_up, e_down = src[2, c, up, :], src[2, c, down, :]
            b_sum = src[1, c, up, :] + src[1, c, down, :]
            across, along = a_right[c] - a_left[c], a_down - a_up
            q = state[0, c, here, :]
            lam_q = (
                KEEP * a[c]
                + diffuse * ((a_right[c] + a_left[c]) + (a_up + a_down))
                + (state[1, c, here, :] * across + state[2, c, here, :] * along)
                + SLOPE * ((b_right[c] - b_left[c]) + (e_down - e_up))
            )
            lam_u = (
                KEEP * b[c]
                + diffuse * ((b_right[c] + b_left[c]) + b_sum)
                + q * across
                - coriolis * e[c]
            )
            lam_v = (
                KEEP * e[c]
                + diffuse * ((e_right[c] + e_left[c]) + (e_up + e_down))
                + q * along
                + coriolis * b[c]
            )
            out.append((lam_q, lam_u, lam_v))
        return out

    def adjoint(levels, dense):
        src, dst = lam_a, lam_b
        for s in reversed(range(1, NSTEP)):

            def one(r, src=src, dst=dst, s=s):
                here, at = pl.ds(r, PAD), drop(r)
                out = adjoint_tile(src, levels.at[s], r)
                for c in every:
                    m = mask[c, here, :]
                    push = dense[s - 1, 0, c, at, :] * levels[s, 0, c, here, :]
                    dst[0, c, here, :] = out[c][0] + (push - dense[s - 1, 1, c, at, :])
                    dst[1, c, here, :] = m * out[c][1]
                    dst[2, c, here, :] = m * out[c][2]

            tile_loop(seed_at, n_seed, parts(n_seed), one)
            edges(dst, (0.0, 0.0, 0.0))
            src, dst = dst, src
        return src

    n_row = rows // PAD
    row_unroll = 2 if n_row % 2 == 0 else 1

    def inside(r):
        return pl.ds(pl.multiple_of(r - low, PAD), PAD)

    def block(c):
        return pl.ds(c * LANES, LANES)

    densify(cells, values, dense_x)
    arrive(*halo)

    def to_mask(r):
        here = pl.ds(pl.multiple_of(r, PAD), PAD)
        for c in every:
            mask[c, here, :] = land_i[c, here, :].astype(jnp.float32)

    full = (rows + 2 * PAD) // PAD
    tile_loop(top, full, parts(full), to_mask)
    transform(xr, xt.at[0], top, high + PAD)
    for levels in (xt, yt):
        for at in (0, high + PAD):
            levels[0, :, :, at : at + PAD, :] = jnp.zeros((3, blocks, PAD, LANES), jnp.float32)
    relay(2)
    forward(xt)
    relay(2)
    arrive(*obs_next)
    densify(cells_n, values_n, dense_y)
    relay(2)
    arrive(*direct[:2], *relayed[:2])
    next_up = has_next & has_up
    next_down = has_next & has_down
    next2_up = has_next2 & has_up
    next2_down = has_next2 & has_down
    halo_next = [
        start(strip(yr, head), strip(yr, bottom), above, next_up, next_down),
        start(strip(yr, tail), strip(yr, top), below, next_down, next_up),
    ]
    halo_far = [
        start(strip(zr, head), strip(zr, bottom), above, next2_up, next2_down),
        start(strip(zr, tail), strip(zr, top), below, next2_down, next2_up),
    ]
    relay(n_piece)
    ends = start(
        xt.at[NSTEP, :, :, pl.ds(low, rows), :], prev_end, ahead, has_next, has_prev
    )
    arrive(*direct[2:], *relayed[2:], *halo_next)

    begin(xt, yr, has_next, dense_x, lam_a)
    last = adjoint(xt, dense_x)

    def own(r):
        out = adjoint_tile(last, xt.at[0], r)
        at = inside(r)
        for c in every:
            gradient[0, at, block(c)] = out[c][0]
            gradient[1, at, block(c)] = HALF * out[c][1]
            gradient[2, at, block(c)] = HALF * out[c][2]

    tile_loop(low, n_row, row_unroll, own)

    transform(yr, yt.at[0], top, high + PAD)
    forward(yt)
    arrive(*halo_far)
    begin(yt, zr, has_next2, dense_y, lam_a)
    last = adjoint(yt, dense_y)

    def raw_end(ref, f, c, here):
        value = ref[f, c, here, :]
        return value - 1.0 if f == 0 else (1.0 / HALF) * value

    def other(r):
        out = adjoint_tile(last, yt.at[0], r)
        here = pl.ds(pl.multiple_of(r, PAD), PAD)
        at = inside(r)
        for c in every:
            for f in range(3):
                state = yr[f, c, here, :]
                end = raw_end(xt.at[NSTEP], f, c, here)
                lam = out[c][f] if f == 0 else HALF * out[c][f]
                grad = defect_weight * (state - end) + lam
                nexts[f, at, block(c)] = jnp.where(has_next, state - step_length * grad, end)

    tile_loop(low, n_row, row_unroll, other)

    arrive(ends)
    for entry in loads[n_early:]:
        entry.wait()

    def finish(r):
        here = pl.ds(pl.multiple_of(r, PAD), PAD)
        at = inside(r)
        for c in every:
            for f in range(3):
                before = jnp.where(
                    has_prev, raw_end(prev_end, f, c, at), back[f, at, block(c)]
                )
                defect = xr[f, c, here, :] - before
                gradient[f, at, block(c)] = gradient[f, at, block(c)] + defect_weight * defect

    tile_loop(low, n_row, 1, finish)

    for entry, sends in started:

        @pl.when(sends)
        def _(entry=entry):
            entry.wait_send()


def solution(mesh):
    n_tm, n_sp = mesh.shape["tm"], mesh.shape["space"]

    def local(states, background, obs_cells, obs_values, land_mask):
        _, fields, rows, cols = states.shape
        padded = rows + 4 * PAD
        blocks = cols // LANES
        block = pltpu.VMEM((fields, rows, cols), jnp.float32)
        f32 = functools.partial(pltpu.VMEM, dtype=jnp.float32)
        i32 = functools.partial(pltpu.VMEM, dtype=jnp.int32)
        n_copy = 11 + 3 * (rows // PAD)
        gradient, nexts = pl.pallas_call(
            functools.partial(kernel, n_tm, n_sp),
            out_shape=(block, block),
            in_specs=[pl.BlockSpec(memory_space=pl.ANY)] * 5,
            out_specs=(pl.BlockSpec(memory_space=pltpu.VMEM),) * 2,
            scratch_shapes=[
                f32((fields, blocks, padded, LANES)),
                f32((fields, blocks, padded, LANES)),
                f32((fields, blocks, padded, LANES)),
                f32((fields, blocks, rows, LANES)),
                f32((NSTEP + 1, fields, blocks, padded, LANES)),
                f32((NSTEP + 1, fields, blocks, padded, LANES)),
                f32((fields, blocks, padded, LANES)),
                f32((fields, blocks, padded, LANES)),
                i32((blocks, padded, LANES)),
                f32((blocks, padded, LANES)),
                f32((NSTEP, 2, blocks, rows + PAD, LANES)),
                f32((NSTEP, 2, blocks, rows + PAD, LANES)),
                f32((fields, rows, cols)),
                i32(obs_cells.shape[1:]),
                f32(obs_values.shape[1:]),
                i32(obs_cells.shape[1:]),
                f32(obs_values.shape[1:]),
                pltpu.SemaphoreType.DMA((2 * blocks + 3,)),
                pltpu.SemaphoreType.DMA((n_copy,)),
                pltpu.SemaphoreType.DMA((n_copy,)),
            ],
            compiler_params=pltpu.CompilerParams(
                collective_id=0, has_side_effects=True, vmem_limit_bytes=44 * 2**20
            ),
        )(states[0], background, obs_cells[0], obs_values[0], land_mask)
        return gradient[None], nexts[None]

    in_specs = (
        P("tm", None, "space", None),
        P(None, "space", None),
        P("tm", None, None),
        P("tm", None, None),
        P("space", None),
    )
    out_specs = (P("tm", None, "space", None), P("tm", None, "space", None))
    return jax.shard_map(local, mesh=mesh, in_specs=in_specs, out_specs=out_specs, check_vma=False)
```

```python
import functools

import jax
import jax.numpy as jnp
from jax import lax
from jax.experimental import pallas as pl
from jax.experimental.pallas import tpu as pltpu
from jax.sharding import PartitionSpec as P

NSTEP = 4
PAD = 8
LANES = 128
DETOUR = 3

advect = 0.25
gravity = 1.0
coriolis = 0.1
diffuse = 0.1
defect_weight = 2.0
obs_weight = 4.0
step_length = 0.1

KEEP = 1.0 - 4.0 * diffuse
HALF = advect / 2.0
SLOPE = HALF * (advect * gravity / 2.0)

MESH = pl.DeviceIdType.MESH


def kernel(
    n_tm,
    n_sp,
    states,
    background,
    cells_h,
    values_h,
    land,
    gradient,
    nexts,
    xr,
    yr,
    zr,
    cr,
    prev_end,
    xt,
    yt,
    ct,
    lam_a,
    lam_b,
    land_i,
    mask,
    dense_x,
    dense_y,
    back,
    cells,
    values,
    cells_n,
    values_n,
    load,
    send,
    recv,
):
    rows, cols = states.shape[1], states.shape[2]
    blocks = cols // LANES
    tm, sp = lax.axis_index("tm"), lax.axis_index("space")
    low, high = 2 * PAD, 2 * PAD + rows
    half_pad = PAD // 2
    has_next, has_next2 = tm < n_tm - 1, tm < n_tm - 2
    has_prev, has_prev2 = tm > 0, tm > 1
    has_up, has_down = sp > 0, sp < n_sp - 1
    every = range(blocks)

    loads = []

    def fetch(src, dst):
        entry = pltpu.make_async_copy(src, dst, load.at[len(loads)])
        entry.start()
        loads.append(entry)

    for c in every:
        part = pl.ds(c * LANES, LANES)
        fetch(states.at[:, :, part], xr.at[:, c, low:high, :])
    n_state = len(loads)
    for c in every:
        part = pl.ds(c * LANES, LANES)
        fetch(land.at[:, part], land_i.at[c, low:high, :])
    fetch(cells_h, cells)
    fetch(values_h, values)
    n_early = len(loads)
    fetch(background, back)

    for start in (0, PAD, high, high + PAD):
        blank = jnp.zeros((3, blocks, PAD, LANES), jnp.float32)
        for ref in (xr, yr, zr, cr):
            ref[:, :, start : start + PAD, :] = blank
        land_i[:, start : start + PAD, :] = jnp.zeros((blocks, PAD, LANES), jnp.int32)

    barrier = pltpu.get_barrier_semaphore()
    near = (
        (has_up, (tm, sp - 1)),
        (has_down, (tm, sp + 1)),
        (has_prev, (tm - 1, sp)),
        (has_next, (tm + 1, sp)),
        (has_prev2, (tm - 2, sp)),
        (has_next2, (tm + 2, sp)),
    )
    if n_tm > DETOUR:
        near += ((tm == 0, (tm + DETOUR, sp)), (tm == DETOUR, (tm - DETOUR, sp)))
    for there, device in near:

        @pl.when(there)
        def _(device=device):
            pl.semaphore_signal(barrier, inc=1, device_id=device, device_id_type=MESH)

    for entry in loads[:n_early]:
        entry.wait()
    pl.semaphore_wait(barrier, sum(there.astype(jnp.int32) for there, _ in near))

    started = []

    def start(src, dst, device, sends, receives):
        index = len(started)
        entry = pltpu.make_async_remote_copy(
            src_ref=src,
            dst_ref=dst,
            send_sem=send.at[index],
            recv_sem=recv.at[index],
            device_id=device,
            device_id_type=MESH,
        )

        @pl.when(sends)
        def _():
            entry.start()

        started.append((entry, sends))
        return entry, receives

    def arrive(*pairs):
        for entry, receives in pairs:

            @pl.when(receives)
            def _(entry=entry):
                entry.wait_recv()

    def strip(ref, at):
        return ref.at[:, :, pl.ds(at, PAD), :]

    above, below = (tm, sp - 1), (tm, sp + 1)
    back1, back2 = (tm - 1, sp), (tm - 2, sp)
    ahead, ahead2 = (tm + 1, sp), (tm + 2, sp)
    top, bottom, head, tail = PAD, high, low, high - PAD

    halo = [
        start(strip(xr, head), strip(xr, bottom), above, has_up, has_down),
        start(strip(xr, tail), strip(xr, top), below, has_down, has_up),
        start(
            land_i.at[:, pl.ds(head, PAD), :],
            land_i.at[:, pl.ds(bottom, PAD), :],
            above,
            has_up,
            has_down,
        ),
        start(
            land_i.at[:, pl.ds(tail, PAD), :],
            land_i.at[:, pl.ds(top, PAD), :],
            below,
            has_down,
            has_up,
        ),
    ]
    even = lax.rem(tm, 2) == 0
    odd = jnp.logical_not(even)
    obs_next = [
        start(cells, cells_n, back1, has_prev, has_next),
        start(values, values_n, back1, has_prev, has_next),
    ]
    pieces = [low, high - PAD, *range(low + PAD, high - PAD, PAD)]
    n_piece = len(pieces)
    far = [start(strip(xr, p), strip(zr, p), back2, has_prev2, has_next2) for p in pieces]
    direct = [start(strip(xr, p), strip(yr, p), back1, odd, even & has_next) for p in pieces]
    relayed, carried = [], []

    def serve(count):
        for i in range(len(relayed), min(len(relayed) + count, n_piece)):
            p = pieces[i]
            arrive(far[i])
            relayed.append(
                start(strip(zr, p), strip(yr, p), ahead, even & has_next2, odd & has_next)
            )
            arrive(direct[i], relayed[i])
            carried.append(start(strip(yr, p), strip(cr, p), ahead2, has_next2, has_prev2))

    first_row = sp * rows - half_pad
    shift = cols.bit_length() - 1
    tall = rows + PAD
    wide = min(2 * LANES, cols)
    wide_shift = wide.bit_length() - 1
    level = lax.broadcasted_iota(jnp.int32, (tall, cells_h.shape[1]), 0)
    column = lax.broadcasted_iota(jnp.int32, (wide, cells_h.shape[1]), 0)

    def densify(cells, values, dense, begin_at, end_at):
        def one(s, carry):
            cell = cells[pl.ds(s, 1), :]
            value = values[pl.ds(s, 1), :]
            row = lax.shift_right_logical(cell, shift) - first_row
            col = lax.bitwise_and(cell, cols - 1)
            inside = (row >= 0) & (row < tall)
            group = lax.shift_right_logical(col, wide_shift)
            key = jnp.where(inside, group * tall + row, -1)
            lane = lax.bitwise_and(col, wide - 1)
            spread = jnp.where(column == lane, 1.0, 0.0).astype(jnp.bfloat16)
            upper = value.astype(jnp.bfloat16).astype(jnp.float32)
            lower = value - upper
            for g in range(cols // wide):
                hit = level == key - g * tall
                picks = jnp.concatenate(
                    [
                        jnp.where(hit, 1.0, 0.0),
                        jnp.where(hit, upper, 0.0),
                        jnp.where(hit, lower, 0.0),
                    ],
                    axis=0,
                ).astype(jnp.bfloat16)
                out = lax.dot_general(
                    picks, spread, (((1,), (1,)), ((), ())), preferred_element_type=jnp.float32
                )
                count = obs_weight * out[:tall]
                total = count + obs_weight * (out[tall : 2 * tall] + out[2 * tall :])
                for c in range(wide // LANES):
                    at = g * (wide // LANES) + c
                    dense[s, 0, at] = count[:, c * LANES : (c + 1) * LANES]
                    dense[s, 1, at] = total[:, c * LANES : (c + 1) * LANES]
            return carry

        lax.fori_loop(begin_at, end_at, one, 0)

    lane_at = lax.broadcasted_iota(jnp.int32, (PAD, LANES), 1)
    is_first, is_last = lane_at == 0, lane_at == LANES - 1

    def from_right(tiles):
        turned = [pltpu.roll(tile, LANES - 1, 1) for tile in tiles]
        return [jnp.where(is_last, turned[(c + 1) % blocks], turned[c]) for c in every]

    def from_left(tiles):
        turned = [pltpu.roll(tile, 1, 1) for tile in tiles]
        return [jnp.where(is_first, turned[c - 1], turned[c]) for c in every]

    def tile_loop(begin, count, unroll, body):
        def group(i, carry):
            for j in range(unroll):
                body(begin + (i * unroll + j) * PAD)
            return carry

        lax.fori_loop(0, count // unroll, group, 0)

    def parts(count):
        return max(u for u in (4, 3, 2, 1) if count % u == 0 and u <= 3)

    def edges(ref, fill):
        for there, at in ((has_up, top), (has_down, bottom)):

            @pl.when(jnp.logical_not(there))
            def _(at=at):
                for field in range(3):
                    value = jnp.full((blocks, PAD, LANES), fill[field], jnp.float32)
                    ref[field, :, at : at + PAD, :] = value

    def transform(raw, ref, first, last):
        def one(r):
            r = pl.multiple_of(r, PAD)
            here = pl.ds(r, PAD)
            for c in every:
                ref[0, c, here, :] = 1.0 + raw[0, c, here, :]
                ref[1, c, here, :] = HALF * raw[1, c, here, :]
                ref[2, c, here, :] = HALF * raw[2, c, here, :]

        count = (last - first) // PAD
        tile_loop(first, count, parts(count), one)

    def forward_tile(src, dst, r):
        here, up, down = pl.ds(r, PAD), pl.ds(r - 1, PAD), pl.ds(r + 1, PAD)
        q = [src[0, c, here, :] for c in every]
        u = [src[1, c, here, :] for c in every]
        v = [src[2, c, here, :] for c in every]
        slope = [SLOPE * q[c] for c in every]
        mixed = [diffuse * u[c] for c in every]
        q_right = from_right([q[c] * (diffuse - u[c]) for c in every])
        q_left = from_left([q[c] * (diffuse + u[c]) for c in every])
        u_right = from_right([mixed[c] - slope[c] for c in every])
        u_left = from_left([mixed[c] + slope[c] for c in every])
        v_right = from_right(v)
        v_left = from_left(v)
        for c in every:
            m = mask[c, here, :]
            q_up, q_down = src[0, c, up, :], src[0, c, down, :]
            v_up, v_down = src[2, c, up, :], src[2, c, down, :]
            u_sum = src[1, c, up, :] + src[1, c, down, :]
            dst[0, c, here, :] = (
                KEEP * q[c]
                + (q_right[c] + q_left[c])
                + (q_up * (diffuse + v_up) + q_down * (diffuse - v_down))
            )
            dst[1, c, here, :] = m * (
                KEEP * u[c] + coriolis * v[c] + (u_right[c] + u_left[c]) + diffuse * u_sum
            )
            dst[2, c, here, :] = m * (
                KEEP * v[c]
                - coriolis * u[c]
                + diffuse * ((v_right[c] + v_left[c]) + (v_up + v_down))
                + SLOPE * (q_up - q_down)
            )

    def forward(levels):
        full = (rows + 2 * PAD) // PAD

        def step(s, carry):
            src, dst = levels.at[s], levels.at[s + 1]
            tile_loop(top, full, parts(full), lambda r: forward_tile(src, dst, r))
            edges(dst, (1.0, 0.0, 0.0))
            return carry

        lax.fori_loop(0, NSTEP - 1, step, 0)
        src, dst = levels.at[NSTEP - 1], levels.at[NSTEP]
        count = full - 1
        tile_loop(top + half_pad, count, parts(count), lambda r: forward_tile(src, dst, r))
        edges(dst, (1.0, 0.0, 0.0))

    n_seed = (rows + PAD) // PAD
    seed_at = top + half_pad

    def drop(r):
        return pl.ds(pl.multiple_of(r - seed_at, PAD), PAD)

    def begin(levels, following, there, dense, lam):
        ends = levels.at[NSTEP]
        weight = jnp.where(there, defect_weight, 0.0)

        def one(r):
            here, at = pl.ds(r, PAD), drop(r)
            for c in every:
                m = mask[c, here, :]
                raw = [jnp.where(there, following[f, c, here, :], 0.0) for f in range(3)]
                pull = weight + dense[NSTEP - 1, 0, c, at, :]
                lam[0, c, here, :] = (
                    pull * ends[0, c, here, :]
                    - (weight + dense[NSTEP - 1, 1, c, at, :])
                    - weight * raw[0]
                )
                for f in (1, 2):
                    gap = (weight / (HALF * HALF)) * ends[f, c, here, :]
                    lam[f, c, here, :] = m * (gap - (weight / HALF) * raw[f])

        tile_loop(seed_at, n_seed, parts(n_seed), one)
        edges(lam, (0.0, 0.0, 0.0))

    def adjoint_tile(src, state, r):
        here, up, down = pl.ds(r, PAD), pl.ds(r - 1, PAD), pl.ds(r + 1, PAD)
        a = [src[0, c, here, :] for c in every]
        b = [src[1, c, here, :] for c in every]
        e = [src[2, c, here, :] for c in every]
        a_right, a_left = from_right(a), from_left(a)
        b_right, b_left = from_right(b), from_left(b)
        e_right, e_left = from_right(e), from_left(e)
        out = []
        for c in every:
            a_up, a_down = src[0, c, up, :], src[0, c, down, :]
            e_up, e_down = src[2, c, up, :], src[2, c, down, :]
            b_sum = src[1, c, up, :] + src[1, c, down, :]
            across, along = a_right[c] - a_left[c], a_down - a_up
            q = state[0, c, here, :]
            lam_q = (
                KEEP * a[c]
                + diffuse * ((a_right[c] + a_left[c]) + (a_up + a_down))
                + (state[1, c, here, :] * across + state[2, c, here, :] * along)
                + SLOPE * ((b_right[c] - b_left[c]) + (e_down - e_up))
            )
            lam_u = (
                KEEP * b[c]
                + diffuse * ((b_right[c] + b_left[c]) + b_sum)
                + q * across
                - coriolis * e[c]
            )
            lam_v = (
                KEEP * e[c]
                + diffuse * ((e_right[c] + e_left[c]) + (e_up + e_down))
                + q * along
                + coriolis * b[c]
            )
            out.append((lam_q, lam_u, lam_v))
        return out

    def adjoint(levels, dense):
        src, dst = lam_a, lam_b
        for s in reversed(range(1, NSTEP)):

            def one(r, src=src, dst=dst, s=s):
                here, at = pl.ds(r, PAD), drop(r)
                out = adjoint_tile(src, levels.at[s], r)
                for c in every:
                    m = mask[c, here, :]
                    push = dense[s - 1, 0, c, at, :] * levels[s, 0, c, here, :]
                    dst[0, c, here, :] = out[c][0] + (push - dense[s - 1, 1, c, at, :])
                    dst[1, c, here, :] = m * out[c][1]
                    dst[2, c, here, :] = m * out[c][2]

            tile_loop(seed_at, n_seed, parts(n_seed), one)
            edges(dst, (0.0, 0.0, 0.0))
            src, dst = dst, src
        return src

    n_row = rows // PAD
    row_unroll = 2 if n_row % 2 == 0 else 1

    def inside(r):
        return pl.ds(pl.multiple_of(r - low, PAD), PAD)

    def block(c):
        return pl.ds(c * LANES, LANES)

    densify(cells, values, dense_x, 0, NSTEP)
    arrive(*halo)

    def to_mask(r):
        here = pl.ds(pl.multiple_of(r, PAD), PAD)
        for c in every:
            mask[c, here, :] = land_i[c, here, :].astype(jnp.float32)

    full = (rows + 2 * PAD) // PAD
    tile_loop(top, full, parts(full), to_mask)
    transform(xr, xt.at[0], top, high + PAD)
    for levels in (xt, yt, ct):
        for at in (0, high + PAD):
            levels[0, :, :, at : at + PAD, :] = jnp.zeros((3, blocks, PAD, LANES), jnp.float32)
    serve(1)
    forward(xt)
    serve(1)
    next_up = has_next & has_up
    next_down = has_next & has_down
    next2_up = has_next2 & has_up
    next2_down = has_next2 & has_down
    prev2_up = has_prev2 & has_up
    prev2_down = has_prev2 & has_down
    halo_next = [
        start(strip(yr, head), strip(yr, bottom), above, next_up, next_down),
        start(strip(yr, tail), strip(yr, top), below, next_down, next_up),
    ]
    halo_far = [
        start(strip(zr, head), strip(zr, bottom), above, next2_up, next2_down),
        start(strip(zr, tail), strip(zr, top), below, next2_down, next2_up),
    ]
    arrive(*obs_next)
    serve(1)
    densify(cells_n, values_n, dense_y, 0, NSTEP // 2)
    serve(1)
    densify(cells_n, values_n, dense_y, NSTEP // 2, NSTEP)
    serve(1)
    arrive(*carried[:2])
    halo_carried = [
        start(strip(cr, head), strip(cr, bottom), above, prev2_up, prev2_down),
        start(strip(cr, tail), strip(cr, top), below, prev2_down, prev2_up),
    ]
    serve(n_piece)
    n_far = n_piece * 3 // 8 if n_tm > DETOUR else 0
    via = [
        start(
            strip(xt.at[NSTEP], p),
            strip(prev_end, p - low),
            (tm + DETOUR, sp),
            tm == 0,
            tm == DETOUR,
        )
        for p in pieces[n_piece - n_far :]
    ]
    ends = [
        start(strip(xt.at[NSTEP], p), strip(prev_end, p - low), ahead, tm == 0, tm == 1)
        for p in pieces[: n_piece - n_far]
    ]
    arrive(*halo_next)

    def detour():
        for i, p in enumerate(pieces[n_piece - n_far :]):
            arrive(via[i])
            at = strip(prev_end, p - low)
            ends.append(start(at, at, back2, tm == DETOUR, tm == 1))

    begin(xt, yr, has_next, dense_x, lam_a)
    last = adjoint(xt, dense_x)

    def own(r):
        out = adjoint_tile(last, xt.at[0], r)
        at = inside(r)
        for c in every:
            gradient[0, at, block(c)] = out[c][0]
            gradient[1, at, block(c)] = HALF * out[c][1]
            gradient[2, at, block(c)] = HALF * out[c][2]

    tile_loop(low, n_row, row_unroll, own)

    transform(yr, yt.at[0], top, high + PAD)
    forward(yt)
    arrive(*halo_far)
    begin(yt, zr, has_next2, dense_y, lam_a)
    last = adjoint(yt, dense_y)

    def raw_end(ref, f, c, here):
        value = ref[f, c, here, :]
        return value - 1.0 if f == 0 else (1.0 / HALF) * value

    def other(r):
        out = adjoint_tile(last, yt.at[0], r)
        here = pl.ds(pl.multiple_of(r, PAD), PAD)
        at = inside(r)
        for c in every:
            for f in range(3):
                state = yr[f, c, here, :]
                end = raw_end(xt.at[NSTEP], f, c, here)
                lam = out[c][f] if f == 0 else HALF * out[c][f]
                grad = defect_weight * (state - end) + lam
                nexts[f, at, block(c)] = jnp.where(has_next, state - step_length * grad, end)

    tile_loop(low, n_row, row_unroll, other)

    arrive(*carried[2:], *halo_carried)

    @pl.when(has_prev2)
    def _():
        transform(cr, ct.at[0], top, high + PAD)
        src, dst = ct.at[0], ct.at[1]
        for s in range(NSTEP - 1):
            tile_loop(
                seed_at,
                n_seed,
                parts(n_seed),
                lambda r, src=src, dst=dst: forward_tile(src, dst, r),
            )
            edges(dst, (1.0, 0.0, 0.0))
            src, dst = dst, src
        tile_loop(low, n_row, row_unroll, lambda r: forward_tile(src, dst, r))

    detour()
    arrive(*ends)
    for entry in loads[n_early:]:
        entry.wait()

    def finish(before):
        def one(r):
            here = pl.ds(pl.multiple_of(r, PAD), PAD)
            at = inside(r)
            for c in every:
                for f in range(3):
                    defect = xr[f, c, here, :] - before(f, c, here, at)
                    gradient[f, at, block(c)] = gradient[f, at, block(c)] + defect_weight * defect

        tile_loop(low, n_row, 1, one)

    @pl.when(has_prev2)
    def _():
        finish(lambda f, c, here, at: raw_end(ct.at[NSTEP % 2], f, c, here))

    @pl.when(tm == 1)
    def _():
        finish(lambda f, c, here, at: raw_end(prev_end, f, c, at))

    @pl.when(tm == 0)
    def _():
        finish(lambda f, c, here, at: back[f, at, block(c)])

    for entry, sends in started:

        @pl.when(sends)
        def _(entry=entry):
            entry.wait_send()


def solution(mesh):
    n_tm, n_sp = mesh.shape["tm"], mesh.shape["space"]

    def local(states, background, obs_cells, obs_values, land_mask):
        _, fields, rows, cols = states.shape
        padded = rows + 4 * PAD
        blocks = cols // LANES
        block = pltpu.VMEM((fields, rows, cols), jnp.float32)
        f32 = functools.partial(pltpu.VMEM, dtype=jnp.float32)
        i32 = functools.partial(pltpu.VMEM, dtype=jnp.int32)
        n_copy = 12 + 6 * (rows // PAD)
        gradient, nexts = pl.pallas_call(
            functools.partial(kernel, n_tm, n_sp),
            out_shape=(block, block),
            in_specs=[pl.BlockSpec(memory_space=pl.ANY)] * 5,
            out_specs=(pl.BlockSpec(memory_space=pltpu.VMEM),) * 2,
            scratch_shapes=[
                f32((fields, blocks, padded, LANES)),
                f32((fields, blocks, padded, LANES)),
                f32((fields, blocks, padded, LANES)),
                f32((fields, blocks, padded, LANES)),
                f32((fields, blocks, rows, LANES)),
                f32((NSTEP + 1, fields, blocks, padded, LANES)),
                f32((NSTEP + 1, fields, blocks, padded, LANES)),
                f32((2, fields, blocks, padded, LANES)),
                f32((fields, blocks, padded, LANES)),
                f32((fields, blocks, padded, LANES)),
                i32((blocks, padded, LANES)),
                f32((blocks, padded, LANES)),
                f32((NSTEP, 2, blocks, rows + PAD, LANES)),
                f32((NSTEP, 2, blocks, rows + PAD, LANES)),
                f32((fields, rows, cols)),
                i32(obs_cells.shape[1:]),
                f32(obs_values.shape[1:]),
                i32(obs_cells.shape[1:]),
                f32(obs_values.shape[1:]),
                pltpu.SemaphoreType.DMA((2 * blocks + 3,)),
                pltpu.SemaphoreType.DMA((n_copy,)),
                pltpu.SemaphoreType.DMA((n_copy,)),
            ],
            compiler_params=pltpu.CompilerParams(
                collective_id=0, has_side_effects=True, vmem_limit_bytes=44 * 2**20
            ),
        )(states[0], background, obs_cells[0], obs_values[0], land_mask)
        return gradient[None], nexts[None]

    in_specs = (
        P("tm", None, "space", None),
        P(None, "space", None),
        P("tm", None, None),
        P("tm", None, None),
        P("space", None),
    )
    out_specs = (P("tm", None, "space", None), P("tm", None, "space", None))
    return jax.shard_map(local, mesh=mesh, in_specs=in_specs, out_specs=out_specs, check_vma=False)
```

```python
import functools

import jax
import jax.numpy as jnp
from jax import lax
from jax.experimental import pallas as pl
from jax.experimental.pallas import tpu as pltpu
from jax.sharding import PartitionSpec as P

NSTEP = 4
PAD = 8
LANES = 128
DETOUR = 3
UNROLL = 5

advect = 0.25
gravity = 1.0
coriolis = 0.1
diffuse = 0.1
defect_weight = 2.0
obs_weight = 4.0
step_length = 0.1

KEEP = 1.0 - 4.0 * diffuse
HALF = advect / 2.0
SLOPE = HALF * (advect * gravity / 2.0)

MESH = pl.DeviceIdType.MESH


def kernel(
    n_tm,
    n_sp,
    states,
    background,
    cells_h,
    values_h,
    land,
    gradient,
    nexts,
    xr,
    yr,
    zr,
    cr,
    prev_end,
    xt,
    yt,
    ct,
    lam_x,
    lam_y,
    land_i,
    mask,
    dense_x,
    dense_y,
    back,
    cells,
    values,
    cells_n,
    values_n,
    load,
    send,
    recv,
):
    rows, cols = states.shape[1], states.shape[2]
    blocks = cols // LANES
    tm, sp = lax.axis_index("tm"), lax.axis_index("space")
    low, high = 2 * PAD, 2 * PAD + rows
    half_pad = PAD // 2
    lift = low + half_pad
    has_next, has_next2 = tm < n_tm - 1, tm < n_tm - 2
    has_prev, has_prev2 = tm > 0, tm > 1
    has_up, has_down = sp > 0, sp < n_sp - 1
    every = range(blocks)

    loads = []

    def fetch(src, dst):
        entry = pltpu.make_async_copy(src, dst, load.at[len(loads)])
        entry.start()
        loads.append(entry)

    for c in every:
        part = pl.ds(c * LANES, LANES)
        fetch(states.at[:, :, part], xr.at[:, c, low:high, :])
    n_state = len(loads)
    for c in every:
        part = pl.ds(c * LANES, LANES)
        fetch(land.at[:, part], land_i.at[c, low:high, :])
    fetch(cells_h, cells)
    fetch(values_h, values)
    n_early = len(loads)
    fetch(background, back)

    for at in (PAD, high):
        for ref in (xr, yr, zr, cr):
            ref[:, :, at : at + PAD, :] = jnp.zeros((3, blocks, PAD, LANES), jnp.float32)
        land_i[:, at : at + PAD, :] = jnp.zeros((blocks, PAD, LANES), jnp.int32)

    barrier = pltpu.get_barrier_semaphore()
    near = (
        (has_up, (tm, sp - 1)),
        (has_down, (tm, sp + 1)),
        (has_prev, (tm - 1, sp)),
        (has_next, (tm + 1, sp)),
        (has_prev2, (tm - 2, sp)),
        (has_next2, (tm + 2, sp)),
    )
    if n_tm > DETOUR:
        near += ((tm == 0, (tm + DETOUR, sp)), (tm == DETOUR, (tm - DETOUR, sp)))
    for there, device in near:

        @pl.when(there)
        def _(device=device):
            pl.semaphore_signal(barrier, inc=1, device_id=device, device_id_type=MESH)

    for entry in loads[:n_early]:
        entry.wait()
    pl.semaphore_wait(barrier, sum(there.astype(jnp.int32) for there, _ in near))

    started = []

    def start(src, dst, device, sends, receives):
        index = len(started)
        entry = pltpu.make_async_remote_copy(
            src_ref=src,
            dst_ref=dst,
            send_sem=send.at[index],
            recv_sem=recv.at[index],
            device_id=device,
            device_id_type=MESH,
        )

        @pl.when(sends)
        def _():
            entry.start()

        started.append((entry, sends))
        return entry, receives

    def arrive(*pairs):
        for entry, receives in pairs:

            @pl.when(receives)
            def _(entry=entry):
                entry.wait_recv()

    def strip(ref, at):
        return ref.at[:, :, pl.ds(at, PAD), :]

    above, below = (tm, sp - 1), (tm, sp + 1)
    back1, back2 = (tm - 1, sp), (tm - 2, sp)
    ahead, ahead2 = (tm + 1, sp), (tm + 2, sp)
    top, bottom, head, tail = PAD, high, low, high - PAD

    halo = [
        start(strip(xr, head), strip(xr, bottom), above, has_up, has_down),
        start(strip(xr, tail), strip(xr, top), below, has_down, has_up),
        start(
            land_i.at[:, pl.ds(head, PAD), :],
            land_i.at[:, pl.ds(bottom, PAD), :],
            above,
            has_up,
            has_down,
        ),
        start(
            land_i.at[:, pl.ds(tail, PAD), :],
            land_i.at[:, pl.ds(top, PAD), :],
            below,
            has_down,
            has_up,
        ),
    ]
    even = lax.rem(tm, 2) == 0
    odd = jnp.logical_not(even)
    obs_next = [
        start(cells, cells_n, back1, has_prev, has_next),
        start(values, values_n, back1, has_prev, has_next),
    ]
    pieces = [low, high - PAD, *range(low + PAD, high - PAD, PAD)]
    n_piece = len(pieces)
    far = [start(strip(xr, p), strip(zr, p), back2, has_prev2, has_next2) for p in pieces]
    direct = [start(strip(xr, p), strip(yr, p), back1, odd, even & has_next) for p in pieces]
    relayed, carried = [], []

    def serve(count):
        for i in range(len(relayed), min(len(relayed) + count, n_piece)):
            p = pieces[i]
            arrive(far[i])
            relayed.append(
                start(strip(zr, p), strip(yr, p), ahead, even & has_next2, odd & has_next)
            )
            arrive(direct[i], relayed[i])
            carried.append(start(strip(yr, p), strip(cr, p), ahead2, has_next2, has_prev2))

    first_row = sp * rows - half_pad
    shift = cols.bit_length() - 1
    tall = rows + PAD
    wide = min(2 * LANES, cols)
    wide_shift = wide.bit_length() - 1
    level = lax.broadcasted_iota(jnp.int32, (tall, cells_h.shape[1]), 0)
    column = lax.broadcasted_iota(jnp.int32, (wide, cells_h.shape[1]), 0)

    def densify(cells, values, dense, begin_at, end_at):
        def one(s, carry):
            cell = cells[pl.ds(s, 1), :]
            value = values[pl.ds(s, 1), :]
            row = lax.shift_right_logical(cell, shift) - first_row
            col = lax.bitwise_and(cell, cols - 1)
            inside = (row >= 0) & (row < tall)
            group = lax.shift_right_logical(col, wide_shift)
            key = jnp.where(inside, group * tall + row, -1)
            lane = lax.bitwise_and(col, wide - 1)
            spread = jnp.where(column == lane, 1.0, 0.0).astype(jnp.bfloat16)
            upper = value.astype(jnp.bfloat16).astype(jnp.float32)
            lower = value - upper
            for g in range(cols // wide):
                hit = level == key - g * tall
                picks = jnp.concatenate(
                    [
                        jnp.where(hit, 1.0, 0.0),
                        jnp.where(hit, upper, 0.0),
                        jnp.where(hit, lower, 0.0),
                    ],
                    axis=0,
                ).astype(jnp.bfloat16)
                out = lax.dot_general(
                    picks, spread, (((1,), (1,)), ((), ())), preferred_element_type=jnp.float32
                )
                count = obs_weight * out[:tall]
                total = count + obs_weight * (out[tall : 2 * tall] + out[2 * tall :])
                for c in range(wide // LANES):
                    at = g * (wide // LANES) + c
                    dense[s, 0, at] = count[:, c * LANES : (c + 1) * LANES]
                    dense[s, 1, at] = total[:, c * LANES : (c + 1) * LANES]
            return carry

        lax.fori_loop(begin_at, end_at, one, 0)

    lane_at = lax.broadcasted_iota(jnp.int32, (blocks, PAD, LANES), 2)
    is_first, is_last = lane_at == 0, lane_at == LANES - 1

    def onward(x):
        return jnp.concatenate([x[1:], x[:1]], axis=0)

    def backed(x):
        return jnp.concatenate([x[-1:], x[:-1]], axis=0)

    def from_right(x):
        return pltpu.roll(jnp.where(is_first, onward(x), x), LANES - 1, 2)

    def from_left(x):
        return pltpu.roll(jnp.where(is_last, backed(x), x), 1, 2)

    def turn_right(x):
        turned = pltpu.roll(x, LANES - 1, 2)
        return jnp.where(is_last, onward(turned), turned)

    def turn_left(x):
        turned = pltpu.roll(x, 1, 2)
        return jnp.where(is_first, backed(turned), turned)

    def sweep(first, last, body):
        count = (last - first + PAD - 1) // PAD
        unroll = max(u for u in range(1, UNROLL + 1) if count % u == 0)

        def group(i, carry):
            for j in range(unroll):
                body(i * (unroll * PAD) + (first + j * PAD))
            return carry

        if count == unroll:
            group(0, 0)
        else:
            lax.fori_loop(0, count // unroll, group, 0)

    def at_row(base, r, lag=0):
        start = r + base
        if (base + lag) % PAD == 0 and not isinstance(start, int):
            start = pl.multiple_of(start, PAD)
        return pl.ds(start, PAD)

    def edges(ref, fill, head_end=True, tail_end=True):
        for there, row, use in ((has_up, -PAD, head_end), (has_down, rows, tail_end)):
            if not use:
                continue

            @pl.when(jnp.logical_not(there))
            def _(row=row):
                for field in range(3):
                    value = jnp.full((blocks, PAD, LANES), fill[field], jnp.float32)
                    ref[field, :, lift + row : lift + row + PAD, :] = value

    def transform(raw, ref, first, last):
        def one(r):
            here, there = at_row(low, r), pl.ds(r + lift, PAD)
            ref[0, :, there, :] = 1.0 + raw[0, :, here, :]
            ref[1, :, there, :] = HALF * raw[1, :, here, :]
            ref[2, :, there, :] = HALF * raw[2, :, here, :]

        sweep(first, last, one)

    def forward_tile(src, r):
        r = r + lift
        here, up, down = pl.ds(r, PAD), pl.ds(r - 1, PAD), pl.ds(r + 1, PAD)
        q, u, v = [src[f, :, here, :] for f in range(3)]
        q_up, q_down = src[0, :, up, :], src[0, :, down, :]
        v_up, v_down = src[2, :, up, :], src[2, :, down, :]
        u_sum = src[1, :, up, :] + src[1, :, down, :]
        m = mask[:, here, :]
        slope, mixed = SLOPE * q, diffuse * u
        q_new = (
            KEEP * q
            + (from_right(q * (diffuse - u)) + from_left(q * (diffuse + u)))
            + (q_up * (diffuse + v_up) + q_down * (diffuse - v_down))
        )
        u_new = m * (
            KEEP * u
            + coriolis * v
            + (from_right(mixed - slope) + from_left(mixed + slope))
            + diffuse * u_sum
        )
        v_new = m * (
            KEEP * v
            - coriolis * u
            + diffuse * ((from_right(v) + from_left(v)) + (v_up + v_down))
            + SLOPE * (q_up - q_down)
        )
        return q_new, u_new, v_new

    def forward(src, dst, first, last, head_end, tail_end):
        def one(r):
            out = forward_tile(src, r)
            here = pl.ds(r + lift, PAD)
            for f in range(3):
                dst[f, :, here, :] = out[f]

        sweep(first, last, one)
        edges(dst, (1.0, 0.0, 0.0), head_end, tail_end)

    def seed(levels, following, there, dense, lam, first, last, head_end, tail_end):
        ends = levels.at[NSTEP]
        weight = jnp.where(there, defect_weight, 0.0)

        def one(r):
            here, raw_at, at = at_row(lift, r, half_pad), pl.ds(r + low, PAD), drop(r)
            m = mask[:, here, :]
            raw = [jnp.where(there, following[f, :, raw_at, :], 0.0) for f in range(3)]
            pull = weight + dense[NSTEP - 1, 0, :, at, :]
            lam[0, :, here, :] = (
                pull * ends[0, :, here, :]
                - (weight + dense[NSTEP - 1, 1, :, at, :])
                - weight * raw[0]
            )
            for f in (1, 2):
                gap = (weight / (HALF * HALF)) * ends[f, :, here, :]
                lam[f, :, here, :] = m * (gap - (weight / HALF) * raw[f])

        sweep(first, last, one)
        edges(lam, (0.0, 0.0, 0.0), head_end, tail_end)

    def drop(r):
        return pl.ds(r + half_pad, PAD)

    def adjoint_tile(src, state, r):
        r = r + lift
        here, up, down = pl.ds(r, PAD), pl.ds(r - 1, PAD), pl.ds(r + 1, PAD)
        a, b, e = [src[f, :, here, :] for f in range(3)]
        a_right, a_left = turn_right(a), turn_left(a)
        b_right, b_left = turn_right(b), turn_left(b)
        e_right, e_left = turn_right(e), turn_left(e)
        a_up, a_down = src[0, :, up, :], src[0, :, down, :]
        e_up, e_down = src[2, :, up, :], src[2, :, down, :]
        b_sum = src[1, :, up, :] + src[1, :, down, :]
        across, along = a_right - a_left, a_down - a_up
        q = state[0, :, here, :]
        lam_q = (
            KEEP * a
            + diffuse * ((a_right + a_left) + (a_up + a_down))
            + (state[1, :, here, :] * across + state[2, :, here, :] * along)
            + SLOPE * ((b_right - b_left) + (e_down - e_up))
        )
        lam_u = (
            KEEP * b + diffuse * ((b_right + b_left) + b_sum) + q * across - coriolis * e
        )
        lam_v = (
            KEEP * e
            + diffuse * ((e_right + e_left) + (e_up + e_down))
            + q * along
            + coriolis * b
        )
        return lam_q, lam_u, lam_v

    def adjoint(levels, dense, lam, s, first, last, head_end, tail_end):
        src, dst = lam.at[s], lam.at[s - 1]

        def one(r):
            here, at = pl.ds(r + lift, PAD), drop(r)
            out = adjoint_tile(src, levels.at[s], r)
            m = mask[:, here, :]
            push = dense[s - 1, 0, :, at, :] * levels[s, 0, :, here, :]
            dst[0, :, here, :] = out[0] + (push - dense[s - 1, 1, :, at, :])
            dst[1, :, here, :] = m * out[1]
            dst[2, :, here, :] = m * out[2]

        sweep(first, last, one)
        edges(dst, (0.0, 0.0, 0.0), head_end, tail_end)

    split = rows // 2
    overlap = half_pad

    def backward(levels, following, there, dense, lam, final, upper):
        stack = lam
        lam = [stack.at[s] for s in range(NSTEP)]
        if upper:
            first, last = -overlap, split - overlap
            seed(levels, following, there, dense, lam[NSTEP - 1], first, last, True, False)
            for s in reversed(range(1, NSTEP)):
                adjoint(levels, dense, stack, s, first, last, True, False)
            sweep(0, split - PAD, lambda r: final(adjoint_tile(lam[0], levels.at[0], r), r))
        else:
            first, last = split - overlap, rows + overlap
            seed(levels, following, there, dense, lam[NSTEP - 1], first, last, False, True)
            for s in reversed(range(1, NSTEP)):
                lag = NSTEP - s
                adjoint(levels, dense, stack, s, first - lag, last - lag, False, True)
            sweep(split - PAD, rows, lambda r: final(adjoint_tile(lam[0], levels.at[0], r), r))

    def block(c):
        return pl.ds(c * LANES, LANES)

    def raw_end(value, f):
        return value - 1.0 if f == 0 else (1.0 / HALF) * value

    def put(ref, f, at, value):
        for c in every:
            ref[f, at, block(c)] = value[c]

    def own(out, r):
        for f in range(3):
            put(gradient, f, at_row(0, r), out[f] if f == 0 else HALF * out[f])

    def other(out, r):
        here, lifted = at_row(low, r), pl.ds(r + lift, PAD)
        for f in range(3):
            state = yr[f, :, here, :]
            end = raw_end(xt[NSTEP, f, :, lifted, :], f)
            lam = out[f] if f == 0 else HALF * out[f]
            grad = defect_weight * (state - end) + lam
            put(
                nexts, f, at_row(0, r), jnp.where(has_next, state - step_length * grad, end)
            )

    def to_mask(r):
        here, there = at_row(low, r), pl.ds(r + lift, PAD)
        mask[:, there, :] = land_i[:, here, :].astype(jnp.float32)

    densify(cells, values, dense_x, 0, NSTEP)
    arrive(*halo)
    sweep(-PAD, rows + PAD, to_mask)
    transform(xr, xt.at[0], -PAD, rows + PAD)
    serve(1)

    def own_step(s, carry):
        forward(xt.at[s], xt.at[s + 1], -PAD, rows + PAD, True, True)
        return carry

    lax.fori_loop(0, NSTEP // 2, own_step, 0)
    serve(1)
    next_up = has_next & has_up
    next_down = has_next & has_down
    next2_up = has_next2 & has_up
    next2_down = has_next2 & has_down
    prev2_up = has_prev2 & has_up
    prev2_down = has_prev2 & has_down
    halo_next = [
        start(strip(yr, head), strip(yr, bottom), above, next_up, next_down),
        start(strip(yr, tail), strip(yr, top), below, next_down, next_up),
    ]
    halo_far = [
        start(strip(zr, head), strip(zr, bottom), above, next2_up, next2_down),
        start(strip(zr, tail), strip(zr, top), below, next2_down, next2_up),
    ]
    lax.fori_loop(NSTEP // 2, NSTEP, own_step, 0)
    serve(1)
    arrive(*obs_next)
    densify(cells_n, values_n, dense_y, 0, NSTEP // 2)
    serve(1)
    densify(cells_n, values_n, dense_y, NSTEP // 2, NSTEP)
    serve(split // PAD + 1 - len(relayed))
    arrive(*halo_next)

    backward(xt, yr, has_next, dense_x, lam_x, own, True)
    serve(1)
    arrive(*carried[:2])
    halo_carried = [
        start(strip(cr, head), strip(cr, bottom), above, prev2_up, prev2_down),
        start(strip(cr, tail), strip(cr, top), below, prev2_down, prev2_up),
    ]
    transform(yr, yt.at[0], -PAD, split)
    for s in range(NSTEP):
        last = split - 1 - s
        first = -overlap if s == NSTEP - 1 else last - (split + PAD)
        forward(yt.at[s], yt.at[s + 1], first, last, True, False)
    serve(1)
    arrive(*halo_far)
    backward(yt, zr, has_next2, dense_y, lam_y, other, True)
    serve(n_piece)
    n_far = n_piece * 3 // 8 if n_tm > DETOUR else 0

    def finish_source(p):
        return xt.at[NSTEP, :, :, pl.ds(p + half_pad, PAD), :]

    via = [
        start(
            finish_source(p), strip(prev_end, p - low), (tm + DETOUR, sp), tm == 0, tm == DETOUR
        )
        for p in pieces[n_piece - n_far :]
    ]
    ends = [
        start(finish_source(p), strip(prev_end, p - low), ahead, tm == 0, tm == 1)
        for p in pieces[: n_piece - n_far]
    ]

    passed = []

    def detour(count):
        for i in range(len(passed), min(len(passed) + count, n_far)):
            arrive(via[i])
            at = strip(prev_end, pieces[n_piece - n_far + i] - low)
            passed.append(start(at, at, back2, tm == DETOUR, tm == 1))

    backward(xt, yr, has_next, dense_x, lam_x, own, False)
    transform(yr, yt.at[0], split, rows + PAD)
    for s in range(NSTEP):
        first = split - 1 - s
        forward(yt.at[s], yt.at[s + 1], first, rows + PAD - 1 - s, False, True)
    backward(yt, zr, has_next2, dense_y, lam_y, other, False)
    detour(1)
    arrive(*carried[2:], *halo_carried)

    @pl.when(has_prev2)
    def _():
        transform(cr, ct.at[0], -PAD, rows + PAD)
        forward(ct.at[0], ct.at[1], -overlap, rows + overlap, True, True)
        forward(ct.at[1], ct.at[0], -overlap, rows + overlap, True, True)

    detour(1)

    def settle(f, r, before):
        at = at_row(0, r)
        for c in every:
            defect = xr[f, c, at_row(low, r), :] - before(c)
            gradient[f, at, block(c)] = gradient[f, at, block(c)] + defect_weight * defect

    @pl.when(has_prev2)
    def _():
        forward(ct.at[0], ct.at[1], -overlap, rows + overlap, True, True)

        def one(r):
            out = forward_tile(ct.at[1], r)
            for f in range(3):
                end = raw_end(out[f], f)
                settle(f, r, lambda c, end=end: end[c])

        sweep(0, rows, one)

    detour(n_piece)
    arrive(*ends, *passed)
    for entry in loads[n_early:]:
        entry.wait()

    def plain(before):
        def one(r):
            for f in range(3):
                settle(f, r, lambda c, f=f: before(f, c, at_row(0, r)))

        sweep(0, rows, one)

    @pl.when(tm == 1)
    def _():
        plain(lambda f, c, at: raw_end(prev_end[f, c, at, :], f))

    @pl.when(tm == 0)
    def _():
        plain(lambda f, c, at: back[f, at, block(c)])

    for entry, sends in started:

        @pl.when(sends)
        def _(entry=entry):
            entry.wait_send()


def solution(mesh):
    n_tm, n_sp = mesh.shape["tm"], mesh.shape["space"]

    def local(states, background, obs_cells, obs_values, land_mask):
        _, fields, rows, cols = states.shape
        padded = rows + 4 * PAD
        lifted = padded + PAD
        blocks = cols // LANES
        block = pltpu.VMEM((fields, rows, cols), jnp.float32)
        f32 = functools.partial(pltpu.VMEM, dtype=jnp.float32)
        i32 = functools.partial(pltpu.VMEM, dtype=jnp.int32)
        n_copy = 12 + 6 * (rows // PAD)
        gradient, nexts = pl.pallas_call(
            functools.partial(kernel, n_tm, n_sp),
            out_shape=(block, block),
            in_specs=[pl.BlockSpec(memory_space=pltpu.HBM)] * 5,
            out_specs=(pl.BlockSpec(memory_space=pltpu.VMEM),) * 2,
            scratch_shapes=[
                f32((fields, blocks, padded, LANES)),
                f32((fields, blocks, padded, LANES)),
                f32((fields, blocks, padded, LANES)),
                f32((fields, blocks, padded, LANES)),
                f32((fields, blocks, rows, LANES)),
                f32((NSTEP + 1, fields, blocks, lifted, LANES)),
                f32((NSTEP + 1, fields, blocks, lifted, LANES)),
                f32((2, fields, blocks, lifted, LANES)),
                f32((NSTEP, fields, blocks, lifted, LANES)),
                f32((NSTEP, fields, blocks, lifted, LANES)),
                i32((blocks, padded, LANES)),
                f32((blocks, lifted, LANES)),
                f32((NSTEP, 2, blocks, rows + PAD, LANES)),
                f32((NSTEP, 2, blocks, rows + PAD, LANES)),
                f32((fields, rows, cols)),
                i32(obs_cells.shape[1:]),
                f32(obs_values.shape[1:]),
                i32(obs_cells.shape[1:]),
                f32(obs_values.shape[1:]),
                pltpu.SemaphoreType.DMA((2 * blocks + 3,)),
                pltpu.SemaphoreType.DMA((n_copy,)),
                pltpu.SemaphoreType.DMA((n_copy,)),
            ],
            compiler_params=pltpu.CompilerParams(
                collective_id=0,
                has_side_effects=True,
                vmem_limit_bytes=56 * 2**20,
            ),
        )(*[
            pltpu.with_memory_space_constraint(x, pltpu.HBM)
            for x in (states[0], background, obs_cells[0], obs_values[0], land_mask)
        ])
        return gradient[None], nexts[None]

    in_specs = (
        P("tm", None, "space", None),
        P(None, "space", None),
        P("tm", None, None),
        P("tm", None, None),
        P("space", None),
    )
    out_specs = (P("tm", None, "space", None), P("tm", None, "space", None))
    return jax.shard_map(local, mesh=mesh, in_specs=in_specs, out_specs=out_specs, check_vma=False)
```

```python
import functools

import jax
import jax.numpy as jnp
from jax import lax
from jax.experimental import pallas as pl
from jax.experimental.pallas import tpu as pltpu
from jax.sharding import PartitionSpec as P

NSTEP = 4
PAD = 8
LANES = 128
DETOUR = 3
UNROLL = 5
LEAD = 2
VIA = 2

advect = 0.25
gravity = 1.0
coriolis = 0.1
diffuse = 0.1
defect_weight = 2.0
obs_weight = 4.0
step_length = 0.1

KEEP = 1.0 - 4.0 * diffuse
HALF = advect / 2.0
SLOPE = HALF * (advect * gravity / 2.0)

MESH = pl.DeviceIdType.MESH


def kernel(
    n_tm,
    n_sp,
    states,
    background,
    cells_h,
    values_h,
    land,
    gradient,
    nexts,
    xr,
    yr,
    zr,
    cr,
    prev_end,
    xt,
    yt,
    ct,
    lam_x,
    lam_y,
    land_i,
    mask,
    dense_x,
    dense_y,
    back,
    cells,
    values,
    cells_n,
    values_n,
    load,
    send,
    recv,
):
    rows, cols = states.shape[1], states.shape[2]
    blocks = cols // LANES
    tm, sp = lax.axis_index("tm"), lax.axis_index("space")
    low, high = 2 * PAD, 2 * PAD + rows
    half_pad = PAD // 2
    lift = low + half_pad
    has_next, has_next2 = tm < n_tm - 1, tm < n_tm - 2
    has_prev, has_prev2 = tm > 0, tm > 1
    has_up, has_down = sp > 0, sp < n_sp - 1
    every = range(blocks)

    loads = []

    def fetch(src, dst):
        entry = pltpu.make_async_copy(src, dst, load.at[len(loads)])
        entry.start()
        loads.append(entry)

    for c in every:
        part = pl.ds(c * LANES, LANES)
        fetch(states.at[:, :, part], xr.at[:, c, low:high, :])
    n_state = len(loads)
    for c in every:
        part = pl.ds(c * LANES, LANES)
        fetch(land.at[:, part], land_i.at[c, low:high, :])
    fetch(cells_h, cells)
    fetch(values_h, values)
    n_early = len(loads)
    fetch(background, back)

    for at in (PAD, high):
        for ref in (xr, yr, zr, cr):
            ref[:, :, at : at + PAD, :] = jnp.zeros((3, blocks, PAD, LANES), jnp.float32)
        land_i[:, at : at + PAD, :] = jnp.zeros((blocks, PAD, LANES), jnp.int32)

    barrier = pltpu.get_barrier_semaphore()
    near = (
        (has_up, (tm, sp - 1)),
        (has_down, (tm, sp + 1)),
        (has_prev, (tm - 1, sp)),
        (has_next, (tm + 1, sp)),
        (has_prev2, (tm - 2, sp)),
        (has_next2, (tm + 2, sp)),
    )
    if n_tm > DETOUR:
        near += ((tm == 0, (tm + DETOUR, sp)), (tm == DETOUR, (tm - DETOUR, sp)))
    for there, device in near:

        @pl.when(there)
        def _(device=device):
            pl.semaphore_signal(barrier, inc=1, device_id=device, device_id_type=MESH)

    for entry in loads[:n_early]:
        entry.wait()
    pl.semaphore_wait(barrier, sum(there.astype(jnp.int32) for there, _ in near))

    started = []

    def start(src, dst, device, sends, receives):
        index = len(started)
        entry = pltpu.make_async_remote_copy(
            src_ref=src,
            dst_ref=dst,
            send_sem=send.at[index],
            recv_sem=recv.at[index],
            device_id=device,
            device_id_type=MESH,
        )

        @pl.when(sends)
        def _():
            entry.start()

        started.append((entry, sends))
        return entry, receives

    def arrive(*pairs):
        for entry, receives in pairs:

            @pl.when(receives)
            def _(entry=entry):
                entry.wait_recv()

    def strip(ref, at):
        return ref.at[:, :, pl.ds(at, PAD), :]

    above, below = (tm, sp - 1), (tm, sp + 1)
    back1, back2 = (tm - 1, sp), (tm - 2, sp)
    ahead, ahead2 = (tm + 1, sp), (tm + 2, sp)
    top, bottom, head, tail = PAD, high, low, high - PAD

    halo = [
        start(strip(xr, head), strip(xr, bottom), above, has_up, has_down),
        start(strip(xr, tail), strip(xr, top), below, has_down, has_up),
        start(
            land_i.at[:, pl.ds(head, PAD), :],
            land_i.at[:, pl.ds(bottom, PAD), :],
            above,
            has_up,
            has_down,
        ),
        start(
            land_i.at[:, pl.ds(tail, PAD), :],
            land_i.at[:, pl.ds(top, PAD), :],
            below,
            has_down,
            has_up,
        ),
    ]
    even = lax.rem(tm, 2) == 0
    odd = jnp.logical_not(even)
    obs_next = [
        start(cells, cells_n, back1, has_prev, has_next),
        start(values, values_n, back1, has_prev, has_next),
    ]
    pieces = [low, high - PAD, *range(low + PAD, high - PAD, PAD)]
    n_piece = len(pieces)
    n_lead = LEAD
    n_plain = n_piece - n_lead
    odd_prev2, odd_next2 = odd & has_prev2, odd & has_next2
    even_prev2, even_next2 = even & has_prev2, even & has_next2
    lead, passed_on, far_late = [], [], []

    def lead_off(count):
        for p in pieces[n_plain + len(lead) : min(n_plain + len(lead) + count, n_piece)]:
            lead.append(start(strip(xr, p), strip(cr, p), ahead, even_prev2, odd_prev2))

    lead_off(1)
    far = [
        start(strip(xr, p), strip(zr, p), back2, has_prev2, has_next2) for p in pieces[:n_plain]
    ]
    far += [
        start(strip(xr, p), strip(zr, p), back2, even_prev2, even_next2)
        for p in pieces[n_plain:]
    ]
    direct = [start(strip(xr, p), strip(yr, p), back1, odd, even & has_next) for p in pieces]
    relayed, carried = [], []

    def serve(count):
        for i in range(len(carried), min(len(carried) + count, n_piece)):
            p = pieces[i]
            arrive(far[i])
            if i < n_plain:
                relayed.append(
                    start(strip(zr, p), strip(yr, p), ahead, even_next2, odd & has_next)
                )
                lead_off(1)
                if i < n_lead:
                    arrive(lead[i])
                    q = pieces[n_plain + i]
                    passed_on.append(
                        start(strip(cr, q), strip(yr, q), back2, odd_prev2, odd_next2)
                    )
                    far_late.append(
                        start(strip(xr, q), strip(zr, q), back2, odd_prev2, odd_next2)
                    )
                arrive(direct[i], relayed[i])
                carried.append(start(strip(yr, p), strip(cr, p), ahead2, has_next2, has_prev2))
            else:
                arrive(direct[i], passed_on[i - n_plain])
                carried.append(
                    start(strip(yr, p), strip(cr, p), ahead2, even_next2, even_prev2)
                )

    first_row = sp * rows - half_pad
    shift = cols.bit_length() - 1
    tall = rows + PAD
    wide = min(2 * LANES, cols)
    wide_shift = wide.bit_length() - 1
    level = lax.broadcasted_iota(jnp.int32, (tall, cells_h.shape[1]), 0)
    column = lax.broadcasted_iota(jnp.int32, (wide, cells_h.shape[1]), 0)

    def densify(cells, values, dense, begin_at, end_at):
        def one(s, carry):
            cell = cells[pl.ds(s, 1), :]
            value = values[pl.ds(s, 1), :]
            row = lax.shift_right_logical(cell, shift) - first_row
            col = lax.bitwise_and(cell, cols - 1)
            inside = (row >= 0) & (row < tall)
            group = lax.shift_right_logical(col, wide_shift)
            key = jnp.where(inside, group * tall + row, -1)
            lane = lax.bitwise_and(col, wide - 1)
            spread = jnp.where(column == lane, 1.0, 0.0).astype(jnp.bfloat16)
            upper = value.astype(jnp.bfloat16).astype(jnp.float32)
            lower = value - upper
            for g in range(cols // wide):
                hit = level == key - g * tall
                picks = jnp.concatenate(
                    [
                        jnp.where(hit, 1.0, 0.0),
                        jnp.where(hit, upper, 0.0),
                        jnp.where(hit, lower, 0.0),
                    ],
                    axis=0,
                ).astype(jnp.bfloat16)
                out = lax.dot_general(
                    picks, spread, (((1,), (1,)), ((), ())), preferred_element_type=jnp.float32
                )
                count = obs_weight * out[:tall]
                total = count + obs_weight * (out[tall : 2 * tall] + out[2 * tall :])
                for c in range(wide // LANES):
                    at = g * (wide // LANES) + c
                    dense[s, 0, at] = count[:, c * LANES : (c + 1) * LANES]
                    dense[s, 1, at] = total[:, c * LANES : (c + 1) * LANES]
            return carry

        lax.fori_loop(begin_at, end_at, one, 0)

    lane_at = lax.broadcasted_iota(jnp.int32, (blocks, PAD, LANES), 2)
    is_first, is_last = lane_at == 0, lane_at == LANES - 1

    def onward(x):
        return jnp.concatenate([x[1:], x[:1]], axis=0)

    def backed(x):
        return jnp.concatenate([x[-1:], x[:-1]], axis=0)

    def from_right(x):
        return pltpu.roll(jnp.where(is_first, onward(x), x), LANES - 1, 2)

    def from_left(x):
        return pltpu.roll(jnp.where(is_last, backed(x), x), 1, 2)

    def turn_right(x):
        turned = pltpu.roll(x, LANES - 1, 2)
        return jnp.where(is_last, onward(turned), turned)

    def turn_left(x):
        turned = pltpu.roll(x, 1, 2)
        return jnp.where(is_first, backed(turned), turned)

    def sweep(first, last, body):
        count = (last - first + PAD - 1) // PAD
        unroll = max(u for u in range(1, UNROLL + 1) if count % u == 0)

        def group(i, carry):
            for j in range(unroll):
                body(i * (unroll * PAD) + (first + j * PAD))
            return carry

        if count == unroll:
            group(0, 0)
        else:
            lax.fori_loop(0, count // unroll, group, 0)

    def at_row(base, r, lag=0):
        start = r + base
        if (base + lag) % PAD == 0 and not isinstance(start, int):
            start = pl.multiple_of(start, PAD)
        return pl.ds(start, PAD)

    def edges(ref, fill, head_end=True, tail_end=True):
        for there, row, use in ((has_up, -PAD, head_end), (has_down, rows, tail_end)):
            if not use:
                continue

            @pl.when(jnp.logical_not(there))
            def _(row=row):
                for field in range(3):
                    value = jnp.full((blocks, PAD, LANES), fill[field], jnp.float32)
                    ref[field, :, lift + row : lift + row + PAD, :] = value

    def transform(raw, ref, first, last):
        def one(r):
            here, there = at_row(low, r), pl.ds(r + lift, PAD)
            ref[0, :, there, :] = 1.0 + raw[0, :, here, :]
            ref[1, :, there, :] = HALF * raw[1, :, here, :]
            ref[2, :, there, :] = HALF * raw[2, :, here, :]

        sweep(first, last, one)

    def forward_tile(src, r):
        r = r + lift
        here, up, down = pl.ds(r, PAD), pl.ds(r - 1, PAD), pl.ds(r + 1, PAD)
        q, u, v = [src[f, :, here, :] for f in range(3)]
        q_up, q_down = src[0, :, up, :], src[0, :, down, :]
        v_up, v_down = src[2, :, up, :], src[2, :, down, :]
        u_sum = src[1, :, up, :] + src[1, :, down, :]
        m = mask[:, here, :]
        slope, mixed = SLOPE * q, diffuse * u
        q_new = (
            KEEP * q
            + (from_right(q * (diffuse - u)) + from_left(q * (diffuse + u)))
            + (q_up * (diffuse + v_up) + q_down * (diffuse - v_down))
        )
        u_new = m * (
            KEEP * u
            + coriolis * v
            + (from_right(mixed - slope) + from_left(mixed + slope))
            + diffuse * u_sum
        )
        v_new = m * (
            KEEP * v
            - coriolis * u
            + diffuse * ((from_right(v) + from_left(v)) + (v_up + v_down))
            + SLOPE * (q_up - q_down)
        )
        return q_new, u_new, v_new

    def forward(src, dst, first, last, head_end, tail_end):
        def one(r):
            out = forward_tile(src, r)
            here = pl.ds(r + lift, PAD)
            for f in range(3):
                dst[f, :, here, :] = out[f]

        sweep(first, last, one)
        edges(dst, (1.0, 0.0, 0.0), head_end, tail_end)

    def seed(levels, following, there, dense, lam, first, last, head_end, tail_end):
        ends = levels.at[NSTEP]
        weight = jnp.where(there, defect_weight, 0.0)

        def one(r):
            here, raw_at, at = at_row(lift, r, half_pad), pl.ds(r + low, PAD), drop(r)
            m = mask[:, here, :]
            raw = [jnp.where(there, following[f, :, raw_at, :], 0.0) for f in range(3)]
            pull = weight + dense[NSTEP - 1, 0, :, at, :]
            lam[0, :, here, :] = (
                pull * ends[0, :, here, :]
                - (weight + dense[NSTEP - 1, 1, :, at, :])
                - weight * raw[0]
            )
            for f in (1, 2):
                gap = (weight / (HALF * HALF)) * ends[f, :, here, :]
                lam[f, :, here, :] = m * (gap - (weight / HALF) * raw[f])

        sweep(first, last, one)
        edges(lam, (0.0, 0.0, 0.0), head_end, tail_end)

    def drop(r):
        return pl.ds(r + half_pad, PAD)

    def adjoint_tile(src, state, r):
        r = r + lift
        here, up, down = pl.ds(r, PAD), pl.ds(r - 1, PAD), pl.ds(r + 1, PAD)
        a, b, e = [src[f, :, here, :] for f in range(3)]
        a_right, a_left = turn_right(a), turn_left(a)
        b_right, b_left = turn_right(b), turn_left(b)
        e_right, e_left = turn_right(e), turn_left(e)
        a_up, a_down = src[0, :, up, :], src[0, :, down, :]
        e_up, e_down = src[2, :, up, :], src[2, :, down, :]
        b_sum = src[1, :, up, :] + src[1, :, down, :]
        across, along = a_right - a_left, a_down - a_up
        q = state[0, :, here, :]
        lam_q = (
            KEEP * a
            + diffuse * ((a_right + a_left) + (a_up + a_down))
            + (state[1, :, here, :] * across + state[2, :, here, :] * along)
            + SLOPE * ((b_right - b_left) + (e_down - e_up))
        )
        lam_u = (
            KEEP * b + diffuse * ((b_right + b_left) + b_sum) + q * across - coriolis * e
        )
        lam_v = (
            KEEP * e
            + diffuse * ((e_right + e_left) + (e_up + e_down))
            + q * along
            + coriolis * b
        )
        return lam_q, lam_u, lam_v

    def adjoint(levels, dense, lam, s, first, last, head_end, tail_end):
        src, dst = lam.at[s], lam.at[s - 1]

        def one(r):
            here, at = pl.ds(r + lift, PAD), drop(r)
            out = adjoint_tile(src, levels.at[s], r)
            m = mask[:, here, :]
            push = dense[s - 1, 0, :, at, :] * levels[s, 0, :, here, :]
            dst[0, :, here, :] = out[0] + (push - dense[s - 1, 1, :, at, :])
            dst[1, :, here, :] = m * out[1]
            dst[2, :, here, :] = m * out[2]

        sweep(first, last, one)
        edges(dst, (0.0, 0.0, 0.0), head_end, tail_end)

    split = rows // 2
    overlap = half_pad

    def backward(levels, following, there, dense, lam, final, upper):
        stack = lam
        lam = [stack.at[s] for s in range(NSTEP)]
        if upper:
            first, last = -overlap, split - overlap
            seed(levels, following, there, dense, lam[NSTEP - 1], first, last, True, False)
            for s in reversed(range(1, NSTEP)):
                adjoint(levels, dense, stack, s, first, last, True, False)
            sweep(0, split - PAD, lambda r: final(adjoint_tile(lam[0], levels.at[0], r), r))
        else:
            first, last = split - overlap, rows + overlap
            seed(levels, following, there, dense, lam[NSTEP - 1], first, last, False, True)
            for s in reversed(range(1, NSTEP)):
                lag = NSTEP - s
                adjoint(levels, dense, stack, s, first - lag, last - lag, False, True)
            sweep(split - PAD, rows, lambda r: final(adjoint_tile(lam[0], levels.at[0], r), r))

    def block(c):
        return pl.ds(c * LANES, LANES)

    def raw_end(value, f):
        return value - 1.0 if f == 0 else (1.0 / HALF) * value

    def put(ref, f, at, value):
        for c in every:
            ref[f, at, block(c)] = value[c]

    def own(out, r):
        for f in range(3):
            put(gradient, f, at_row(0, r), out[f] if f == 0 else HALF * out[f])

    def other(out, r):
        here, lifted = at_row(low, r), pl.ds(r + lift, PAD)
        for f in range(3):
            state = yr[f, :, here, :]
            end = raw_end(xt[NSTEP, f, :, lifted, :], f)
            lam = out[f] if f == 0 else HALF * out[f]
            grad = defect_weight * (state - end) + lam
            put(
                nexts, f, at_row(0, r), jnp.where(has_next, state - step_length * grad, end)
            )

    def to_mask(r):
        here, there = at_row(low, r), pl.ds(r + lift, PAD)
        mask[:, there, :] = land_i[:, here, :].astype(jnp.float32)

    densify(cells, values, dense_x, 0, NSTEP)
    arrive(*halo)
    sweep(-PAD, rows + PAD, to_mask)
    transform(xr, xt.at[0], -PAD, rows + PAD)
    serve(1)

    def own_step(s, carry):
        forward(xt.at[s], xt.at[s + 1], -PAD, rows + PAD, True, True)
        return carry

    lax.fori_loop(0, NSTEP // 2, own_step, 0)
    serve(1)
    next_up = has_next & has_up
    next_down = has_next & has_down
    next2_up = has_next2 & has_up
    next2_down = has_next2 & has_down
    prev2_up = has_prev2 & has_up
    prev2_down = has_prev2 & has_down
    halo_next = [
        start(strip(yr, head), strip(yr, bottom), above, next_up, next_down),
        start(strip(yr, tail), strip(yr, top), below, next_down, next_up),
    ]
    halo_far = [
        start(strip(zr, head), strip(zr, bottom), above, next2_up, next2_down),
        start(strip(zr, tail), strip(zr, top), below, next2_down, next2_up),
    ]
    lax.fori_loop(NSTEP // 2, NSTEP, own_step, 0)
    serve(1)
    arrive(*obs_next)
    densify(cells_n, values_n, dense_y, 0, NSTEP // 2)
    serve(1)
    densify(cells_n, values_n, dense_y, NSTEP // 2, NSTEP)
    serve(split // PAD + 1 - len(carried))
    arrive(*halo_next)

    backward(xt, yr, has_next, dense_x, lam_x, own, True)
    serve(1)
    arrive(*carried[:2])
    halo_carried = [
        start(strip(cr, head), strip(cr, bottom), above, prev2_up, prev2_down),
        start(strip(cr, tail), strip(cr, top), below, prev2_down, prev2_up),
    ]
    transform(yr, yt.at[0], -PAD, split)
    for s in range(NSTEP):
        last = split - 1 - s
        first = -overlap if s == NSTEP - 1 else last - (split + PAD)
        forward(yt.at[s], yt.at[s + 1], first, last, True, False)
    serve(1)
    arrive(*halo_far)
    backward(yt, zr, has_next2, dense_y, lam_y, other, True)
    serve(n_piece)
    n_far = VIA if n_tm > DETOUR else 0

    def finish_source(p):
        return xt.at[NSTEP, :, :, pl.ds(p + half_pad, PAD), :]

    via = [
        start(
            finish_source(p), strip(prev_end, p - low), (tm + DETOUR, sp), tm == 0, tm == DETOUR
        )
        for p in pieces[n_piece - n_far :]
    ]
    ends = [
        start(finish_source(p), strip(prev_end, p - low), ahead, tm == 0, tm == 1)
        for p in pieces[: n_piece - n_far]
    ]

    passed = []

    def detour(count):
        for i in range(len(passed), min(len(passed) + count, n_far)):
            arrive(via[i])
            at = strip(prev_end, pieces[n_piece - n_far + i] - low)
            passed.append(start(at, at, back2, tm == DETOUR, tm == 1))

    backward(xt, yr, has_next, dense_x, lam_x, own, False)
    transform(yr, yt.at[0], split, rows + PAD)
    for s in range(NSTEP):
        first = split - 1 - s
        forward(yt.at[s], yt.at[s + 1], first, rows + PAD - 1 - s, False, True)
    detour(1)
    arrive(*far_late)
    backward(yt, zr, has_next2, dense_y, lam_y, other, False)
    detour(1)
    arrive(*carried[2:], *halo_carried)

    @pl.when(has_prev2)
    def _():
        transform(cr, ct.at[0], -PAD, rows + PAD)
        forward(ct.at[0], ct.at[1], -overlap, rows + overlap, True, True)
        forward(ct.at[1], ct.at[0], -overlap, rows + overlap, True, True)

    detour(1)

    def settle(f, r, before):
        at = at_row(0, r)
        for c in every:
            defect = xr[f, c, at_row(low, r), :] - before(c)
            gradient[f, at, block(c)] = gradient[f, at, block(c)] + defect_weight * defect

    @pl.when(has_prev2)
    def _():
        forward(ct.at[0], ct.at[1], -overlap, rows + overlap, True, True)

        def one(r):
            out = forward_tile(ct.at[1], r)
            for f in range(3):
                end = raw_end(out[f], f)
                settle(f, r, lambda c, end=end: end[c])

        sweep(0, rows, one)

    detour(n_piece)
    arrive(*ends, *passed)
    for entry in loads[n_early:]:
        entry.wait()

    def plain(before):
        def one(r):
            for f in range(3):
                settle(f, r, lambda c, f=f: before(f, c, at_row(0, r)))

        sweep(0, rows, one)

    @pl.when(tm == 1)
    def _():
        plain(lambda f, c, at: raw_end(prev_end[f, c, at, :], f))

    @pl.when(tm == 0)
    def _():
        plain(lambda f, c, at: back[f, at, block(c)])

    for entry, sends in started:

        @pl.when(sends)
        def _(entry=entry):
            entry.wait_send()


def solution(mesh):
    n_tm, n_sp = mesh.shape["tm"], mesh.shape["space"]

    def local(states, background, obs_cells, obs_values, land_mask):
        _, fields, rows, cols = states.shape
        padded = rows + 4 * PAD
        lifted = padded + PAD
        blocks = cols // LANES
        block = pltpu.VMEM((fields, rows, cols), jnp.float32)
        f32 = functools.partial(pltpu.VMEM, dtype=jnp.float32)
        i32 = functools.partial(pltpu.VMEM, dtype=jnp.int32)
        n_copy = 16 + 6 * (rows // PAD) + 3 * LEAD
        gradient, nexts = pl.pallas_call(
            functools.partial(kernel, n_tm, n_sp),
            out_shape=(block, block),
            in_specs=[pl.BlockSpec(memory_space=pltpu.HBM)] * 5,
            out_specs=(pl.BlockSpec(memory_space=pltpu.VMEM),) * 2,
            scratch_shapes=[
                f32((fields, blocks, padded, LANES)),
                f32((fields, blocks, padded, LANES)),
                f32((fields, blocks, padded, LANES)),
                f32((fields, blocks, padded, LANES)),
                f32((fields, blocks, rows, LANES)),
                f32((NSTEP + 1, fields, blocks, lifted, LANES)),
                f32((NSTEP + 1, fields, blocks, lifted, LANES)),
                f32((2, fields, blocks, lifted, LANES)),
                f32((NSTEP, fields, blocks, lifted, LANES)),
                f32((NSTEP, fields, blocks, lifted, LANES)),
                i32((blocks, padded, LANES)),
                f32((blocks, lifted, LANES)),
                f32((NSTEP, 2, blocks, rows + PAD, LANES)),
                f32((NSTEP, 2, blocks, rows + PAD, LANES)),
                f32((fields, rows, cols)),
                i32(obs_cells.shape[1:]),
                f32(obs_values.shape[1:]),
                i32(obs_cells.shape[1:]),
                f32(obs_values.shape[1:]),
                pltpu.SemaphoreType.DMA((2 * blocks + 3,)),
                pltpu.SemaphoreType.DMA((n_copy,)),
                pltpu.SemaphoreType.DMA((n_copy,)),
            ],
            compiler_params=pltpu.CompilerParams(
                collective_id=0,
                has_side_effects=True,
                vmem_limit_bytes=56 * 2**20,
            ),
        )(*[
            pltpu.with_memory_space_constraint(x, pltpu.HBM)
            for x in (states[0], background, obs_cells[0], obs_values[0], land_mask)
        ])
        return gradient[None], nexts[None]

    in_specs = (
        P("tm", None, "space", None),
        P(None, "space", None),
        P("tm", None, None),
        P("tm", None, None),
        P("space", None),
    )
    out_specs = (P("tm", None, "space", None), P("tm", None, "space", None))
    return jax.shard_map(local, mesh=mesh, in_specs=in_specs, out_specs=out_specs, check_vma=False)
```

```python
import functools

import jax
import jax.numpy as jnp
from jax import lax
from jax.experimental import pallas as pl
from jax.experimental.pallas import tpu as pltpu
from jax.sharding import PartitionSpec as P

NSTEP = 4
PAD = 8
LANES = 128
DETOUR = 3
UNROLL = 5
LEAD = 2
VIA = 2
PARTS = (4,)

advect = 0.25
gravity = 1.0
coriolis = 0.1
diffuse = 0.1
defect_weight = 2.0
obs_weight = 4.0
step_length = 0.1

KEEP = 1.0 - 4.0 * diffuse
HALF = advect / 2.0
SLOPE = HALF * (advect * gravity / 2.0)

MESH = pl.DeviceIdType.MESH


def kernel(
    n_tm,
    n_sp,
    states,
    background,
    cells_h,
    values_h,
    land,
    gradient,
    nexts,
    xr,
    yr,
    zr,
    cr,
    prev_end,
    xt,
    yt,
    ct,
    lam_x,
    lam_y,
    land_i,
    mask,
    dense_x,
    dense_y,
    back,
    cells,
    values,
    cells_n,
    values_n,
    load,
    send,
    recv,
):
    rows, cols = states.shape[1], states.shape[2]
    blocks = cols // LANES
    tm, sp = lax.axis_index("tm"), lax.axis_index("space")
    low, high = 2 * PAD, 2 * PAD + rows
    half_pad = PAD // 2
    lift = low + half_pad
    has_next, has_next2 = tm < n_tm - 1, tm < n_tm - 2
    has_prev, has_prev2 = tm > 0, tm > 1
    has_up, has_down = sp > 0, sp < n_sp - 1
    every = range(blocks)

    loads = []

    def fetch(src, dst):
        entry = pltpu.make_async_copy(src, dst, load.at[len(loads)])
        entry.start()
        loads.append(entry)

    for c in every:
        part = pl.ds(c * LANES, LANES)
        fetch(states.at[:, :, part], xr.at[:, c, low:high, :])
    n_state = len(loads)
    for c in every:
        part = pl.ds(c * LANES, LANES)
        fetch(land.at[:, part], land_i.at[c, low:high, :])
    fetch(cells_h, cells)
    fetch(values_h, values)
    n_early = len(loads)
    fetch(background, back)

    for at in (PAD, high):
        for ref in (xr, yr, zr, cr):
            ref[:, :, at : at + PAD, :] = jnp.zeros((3, blocks, PAD, LANES), jnp.float32)
        land_i[:, at : at + PAD, :] = jnp.zeros((blocks, PAD, LANES), jnp.int32)

    barrier = pltpu.get_barrier_semaphore()
    near = (
        (has_up, (tm, sp - 1)),
        (has_down, (tm, sp + 1)),
        (has_prev, (tm - 1, sp)),
        (has_next, (tm + 1, sp)),
        (has_prev2, (tm - 2, sp)),
        (has_next2, (tm + 2, sp)),
    )
    if n_tm > DETOUR:
        near += ((tm == 0, (tm + DETOUR, sp)), (tm == DETOUR, (tm - DETOUR, sp)))
    for there, device in near:

        @pl.when(there)
        def _(device=device):
            pl.semaphore_signal(barrier, inc=1, device_id=device, device_id_type=MESH)

    for entry in loads[:n_early]:
        entry.wait()
    pl.semaphore_wait(barrier, sum(there.astype(jnp.int32) for there, _ in near))

    started = []

    def start(src, dst, device, sends, receives):
        index = len(started)
        entry = pltpu.make_async_remote_copy(
            src_ref=src,
            dst_ref=dst,
            send_sem=send.at[index],
            recv_sem=recv.at[index],
            device_id=device,
            device_id_type=MESH,
        )

        @pl.when(sends)
        def _():
            entry.start()

        started.append((entry, sends))
        return entry, receives

    def arrive(*pairs):
        for entry, receives in pairs:

            @pl.when(receives)
            def _(entry=entry):
                entry.wait_recv()

    def strip(ref, at):
        return ref.at[:, :, pl.ds(at, PAD), :]

    above, below = (tm, sp - 1), (tm, sp + 1)
    back1, back2 = (tm - 1, sp), (tm - 2, sp)
    ahead, ahead2 = (tm + 1, sp), (tm + 2, sp)
    top, bottom, head, tail = PAD, high, low, high - PAD

    halo = [
        start(strip(xr, head), strip(xr, bottom), above, has_up, has_down),
        start(strip(xr, tail), strip(xr, top), below, has_down, has_up),
        start(
            land_i.at[:, pl.ds(head, PAD), :],
            land_i.at[:, pl.ds(bottom, PAD), :],
            above,
            has_up,
            has_down,
        ),
        start(
            land_i.at[:, pl.ds(tail, PAD), :],
            land_i.at[:, pl.ds(top, PAD), :],
            below,
            has_down,
            has_up,
        ),
    ]
    even = lax.rem(tm, 2) == 0
    odd = jnp.logical_not(even)
    obs_next = [
        start(cells, cells_n, back1, has_prev, has_next),
        start(values, values_n, back1, has_prev, has_next),
    ]
    pieces = [low, high - PAD, *range(low + PAD, high - PAD, PAD)]
    n_piece = len(pieces)
    n_lead = LEAD
    n_plain = n_piece - n_lead
    odd_prev2, odd_next2 = odd & has_prev2, odd & has_next2
    even_prev2, even_next2 = even & has_prev2, even & has_next2
    lead, passed_on = [], []

    def lead_off(count):
        for p in pieces[n_plain + len(lead) : min(n_plain + len(lead) + count, n_piece)]:
            lead.append(start(strip(xr, p), strip(cr, p), ahead, even_prev2, odd_prev2))

    lead_off(1)
    far_even = [
        start(strip(xr, p), strip(zr, p), back2, even_prev2, even_next2) for p in pieces
    ]
    far_odd = [
        start(strip(xr, p), strip(zr, p), back2, odd_prev2, odd_next2) for p in pieces[:n_plain]
    ]
    direct = [start(strip(xr, p), strip(yr, p), back1, odd, even & has_next) for p in pieces]
    relayed, from_even, from_odd = [], [], []

    def serve_even(count):
        for i in range(len(from_even), min(len(from_even) + count, n_piece)):
            p = pieces[i]
            arrive(far_even[i])
            if i < n_plain:
                relayed.append(
                    start(strip(zr, p), strip(yr, p), ahead, even_next2, odd & has_next)
                )
                lead_off(1)
            arrive(direct[i])
            from_even.append(
                start(strip(yr, p), strip(cr, p), ahead2, even_next2, even_prev2)
            )

    def serve_lead(count):
        for i in range(len(passed_on), min(len(passed_on) + count, n_lead)):
            p = pieces[n_plain + i]
            arrive(lead[i])
            passed_on.append(start(strip(cr, p), strip(yr, p), back2, odd_prev2, odd_next2))
            far_odd.append(start(strip(xr, p), strip(zr, p), back2, odd_prev2, odd_next2))

    def serve_odd(count):
        for i in range(len(from_odd), min(len(from_odd) + count, n_plain)):
            p = pieces[i]
            arrive(relayed[i])
            from_odd.append(
                start(strip(yr, p), strip(cr, p), ahead2, odd_next2, odd_prev2)
            )

    first_row = sp * rows - half_pad
    shift = cols.bit_length() - 1
    tall = rows + PAD
    wide = min(2 * LANES, cols)
    wide_shift = wide.bit_length() - 1
    level = lax.broadcasted_iota(jnp.int32, (tall, cells_h.shape[1]), 0)
    column = lax.broadcasted_iota(jnp.int32, (wide, cells_h.shape[1]), 0)

    def densify(cells, values, dense, begin_at, end_at):
        def one(s, carry):
            cell = cells[pl.ds(s, 1), :]
            value = values[pl.ds(s, 1), :]
            row = lax.shift_right_logical(cell, shift) - first_row
            col = lax.bitwise_and(cell, cols - 1)
            inside = (row >= 0) & (row < tall)
            group = lax.shift_right_logical(col, wide_shift)
            key = jnp.where(inside, group * tall + row, -1)
            lane = lax.bitwise_and(col, wide - 1)
            spread = jnp.where(column == lane, 1.0, 0.0).astype(jnp.bfloat16)
            upper = value.astype(jnp.bfloat16).astype(jnp.float32)
            lower = value - upper
            for g in range(cols // wide):
                hit = level == key - g * tall
                picks = jnp.concatenate(
                    [
                        jnp.where(hit, 1.0, 0.0),
                        jnp.where(hit, upper, 0.0),
                        jnp.where(hit, lower, 0.0),
                    ],
                    axis=0,
                ).astype(jnp.bfloat16)
                out = lax.dot_general(
                    picks, spread, (((1,), (1,)), ((), ())), preferred_element_type=jnp.float32
                )
                count = obs_weight * out[:tall]
                total = count + obs_weight * (out[tall : 2 * tall] + out[2 * tall :])
                for c in range(wide // LANES):
                    at = g * (wide // LANES) + c
                    dense[s, 0, at] = count[:, c * LANES : (c + 1) * LANES]
                    dense[s, 1, at] = total[:, c * LANES : (c + 1) * LANES]
            return carry

        lax.fori_loop(begin_at, end_at, one, 0)

    lane_at = lax.broadcasted_iota(jnp.int32, (blocks, PAD, LANES), 2)
    is_first, is_last = lane_at == 0, lane_at == LANES - 1

    def onward(x):
        return jnp.concatenate([x[1:], x[:1]], axis=0)

    def backed(x):
        return jnp.concatenate([x[-1:], x[:-1]], axis=0)

    def from_right(x):
        return pltpu.roll(jnp.where(is_first, onward(x), x), LANES - 1, 2)

    def from_left(x):
        return pltpu.roll(jnp.where(is_last, backed(x), x), 1, 2)

    def turn_right(x):
        turned = pltpu.roll(x, LANES - 1, 2)
        return jnp.where(is_last, onward(turned), turned)

    def turn_left(x):
        turned = pltpu.roll(x, 1, 2)
        return jnp.where(is_first, backed(turned), turned)

    def sweep(first, count, body):
        unroll = max(u for u in range(1, UNROLL + 1) if count % u == 0)

        def group(i, carry):
            for j in range(unroll):
                body(i * (unroll * PAD) + (first + j * PAD))
            return carry

        if count == unroll:
            group(0, 0)
        else:
            lax.fori_loop(0, count // unroll, group, 0)

    def at_row(base, r, lag=0):
        start = r + base
        if (base + lag) % PAD == 0 and not isinstance(start, int):
            start = pl.multiple_of(start, PAD)
        return pl.ds(start, PAD)

    def edges(ref, fill, head_end=True, tail_end=True):
        for there, row, use in ((has_up, -PAD, head_end), (has_down, rows, tail_end)):
            if not use:
                continue

            @pl.when(jnp.logical_not(there))
            def _(row=row):
                for field in range(3):
                    value = jnp.full((blocks, PAD, LANES), fill[field], jnp.float32)
                    ref[field, :, lift + row : lift + row + PAD, :] = value

    def transform(raw, ref, first, count):
        def one(r):
            here, there = at_row(low, r), pl.ds(r + lift, PAD)
            ref[0, :, there, :] = 1.0 + raw[0, :, here, :]
            ref[1, :, there, :] = HALF * raw[1, :, here, :]
            ref[2, :, there, :] = HALF * raw[2, :, here, :]

        sweep(first, count, one)

    def forward_tile(src, r):
        r = r + lift
        here, up, down = pl.ds(r, PAD), pl.ds(r - 1, PAD), pl.ds(r + 1, PAD)
        q, u, v = [src[f, :, here, :] for f in range(3)]
        q_up, q_down = src[0, :, up, :], src[0, :, down, :]
        v_up, v_down = src[2, :, up, :], src[2, :, down, :]
        u_sum = src[1, :, up, :] + src[1, :, down, :]
        m = mask[:, here, :]
        slope, mixed = SLOPE * q, diffuse * u
        q_new = (
            KEEP * q
            + (from_right(q * (diffuse - u)) + from_left(q * (diffuse + u)))
            + (q_up * (diffuse + v_up) + q_down * (diffuse - v_down))
        )
        u_new = m * (
            KEEP * u
            + coriolis * v
            + (from_right(mixed - slope) + from_left(mixed + slope))
            + diffuse * u_sum
        )
        v_new = m * (
            KEEP * v
            - coriolis * u
            + diffuse * ((from_right(v) + from_left(v)) + (v_up + v_down))
            + SLOPE * (q_up - q_down)
        )
        return q_new, u_new, v_new

    def forward(src, dst, first, count, head_end, tail_end):
        def one(r):
            out = forward_tile(src, r)
            here = pl.ds(r + lift, PAD)
            for f in range(3):
                dst[f, :, here, :] = out[f]

        sweep(first, count, one)
        edges(dst, (1.0, 0.0, 0.0), head_end, tail_end)

    def seed(levels, following, there, dense, lam, first, count, head_end, tail_end):
        ends = levels.at[NSTEP]
        weight = jnp.where(there, defect_weight, 0.0)

        def one(r):
            here, raw_at, at = pl.ds(r + lift, PAD), pl.ds(r + low, PAD), drop(r)
            m = mask[:, here, :]
            raw = [jnp.where(there, following[f, :, raw_at, :], 0.0) for f in range(3)]
            pull = weight + dense[NSTEP - 1, 0, :, at, :]
            lam[0, :, here, :] = (
                pull * ends[0, :, here, :]
                - (weight + dense[NSTEP - 1, 1, :, at, :])
                - weight * raw[0]
            )
            for f in (1, 2):
                gap = (weight / (HALF * HALF)) * ends[f, :, here, :]
                lam[f, :, here, :] = m * (gap - (weight / HALF) * raw[f])

        sweep(first, count, one)
        edges(lam, (0.0, 0.0, 0.0), head_end, tail_end)

    def drop(r):
        return pl.ds(r + half_pad, PAD)

    def adjoint_tile(src, state, r):
        r = r + lift
        here, up, down = pl.ds(r, PAD), pl.ds(r - 1, PAD), pl.ds(r + 1, PAD)
        a, b, e = [src[f, :, here, :] for f in range(3)]
        a_right, a_left = turn_right(a), turn_left(a)
        b_right, b_left = turn_right(b), turn_left(b)
        e_right, e_left = turn_right(e), turn_left(e)
        a_up, a_down = src[0, :, up, :], src[0, :, down, :]
        e_up, e_down = src[2, :, up, :], src[2, :, down, :]
        b_sum = src[1, :, up, :] + src[1, :, down, :]
        across, along = a_right - a_left, a_down - a_up
        q = state[0, :, here, :]
        lam_q = (
            KEEP * a
            + diffuse * ((a_right + a_left) + (a_up + a_down))
            + (state[1, :, here, :] * across + state[2, :, here, :] * along)
            + SLOPE * ((b_right - b_left) + (e_down - e_up))
        )
        lam_u = (
            KEEP * b + diffuse * ((b_right + b_left) + b_sum) + q * across - coriolis * e
        )
        lam_v = (
            KEEP * e
            + diffuse * ((e_right + e_left) + (e_up + e_down))
            + q * along
            + coriolis * b
        )
        return lam_q, lam_u, lam_v

    def adjoint(levels, dense, lam, s, first, count, head_end, tail_end):
        src, dst = lam.at[s], lam.at[s - 1]

        def one(r):
            here, at = pl.ds(r + lift, PAD), drop(r)
            out = adjoint_tile(src, levels.at[s], r)
            m = mask[:, here, :]
            push = dense[s - 1, 0, :, at, :] * levels[s, 0, :, here, :]
            dst[0, :, here, :] = out[0] + (push - dense[s - 1, 1, :, at, :])
            dst[1, :, here, :] = m * out[1]
            dst[2, :, here, :] = m * out[2]

        sweep(first, count, one)
        edges(dst, (0.0, 0.0, 0.0), head_end, tail_end)

    def rise(levels, begin_row, end_row):
        upper, lower = begin_row is None, end_row > rows
        begin_row = -PAD if upper else begin_row
        count = (end_row - begin_row) // PAD

        for s in range(NSTEP):
            first = begin_row - 1 - s
            forward(levels.at[s], levels.at[s + 1], first, count, upper, lower)

    def fall(levels, following, there, dense, lam, final, begin_row, end_row):
        upper, lower = begin_row is None, end_row > rows
        begin_row = 0 if upper else begin_row
        count = (end_row - begin_row) // PAD
        first = begin_row - half_pad
        seed(levels, following, there, dense, lam.at[NSTEP - 1], first, count, upper, lower)

        for s in reversed(range(1, NSTEP)):
            lag = 0 if upper else NSTEP - s
            adjoint(levels, dense, lam, s, first - lag, count, upper, lower)

        sweep(
            begin_row if upper else begin_row - PAD,
            count - 1 if upper else count,
            lambda r: final(adjoint_tile(lam.at[0], levels.at[0], r), r),
        )

    def block(c):
        return pl.ds(c * LANES, LANES)

    def raw_end(value, f):
        return value - 1.0 if f == 0 else (1.0 / HALF) * value

    def put(ref, f, at, value):
        for c in every:
            ref[f, at, block(c)] = value[c]

    def own(out, r):
        for f in range(3):
            put(gradient, f, at_row(0, r), out[f] if f == 0 else HALF * out[f])

    def other(out, r):
        here, lifted = at_row(low, r), pl.ds(r + lift, PAD)
        for f in range(3):
            state = yr[f, :, here, :]
            end = raw_end(xt[NSTEP, f, :, lifted, :], f)
            lam = out[f] if f == 0 else HALF * out[f]
            grad = defect_weight * (state - end) + lam
            put(
                nexts, f, at_row(0, r), jnp.where(has_next, state - step_length * grad, end)
            )

    def to_mask(r):
        here, there = at_row(low, r), pl.ds(r + lift, PAD)
        mask[:, there, :] = land_i[:, here, :].astype(jnp.float32)

    whole = (rows + 2 * PAD) // PAD
    densify(cells, values, dense_x, 0, NSTEP)
    serve_even(1)
    serve_lead(1)
    arrive(*halo)
    sweep(-PAD, whole, to_mask)
    transform(xr, xt.at[0], -PAD, whole)

    def own_step(s, carry):
        forward(xt.at[s], xt.at[s + 1], -PAD, whole, True, True)
        return carry

    lax.fori_loop(0, NSTEP // 2, own_step, 0)
    serve_even(1)
    serve_lead(1)
    lax.fori_loop(NSTEP // 2, NSTEP, own_step, 0)
    serve_even(1)
    serve_lead(n_lead)
    arrive(*obs_next)
    densify(cells_n, values_n, dense_y, 0, NSTEP // 2)
    serve_even(1)
    serve_odd(2)
    next_up = has_next & has_up
    next_down = has_next & has_down
    next2_up = has_next2 & has_up
    next2_down = has_next2 & has_down
    prev2_up = has_prev2 & has_up
    prev2_down = has_prev2 & has_down
    halo_next = [
        start(strip(yr, head), strip(yr, bottom), above, next_up, next_down),
        start(strip(yr, tail), strip(yr, top), below, next_down, next_up),
    ]
    arrive(far_odd[0], far_odd[1])
    halo_far = [
        start(strip(zr, head), strip(zr, bottom), above, next2_up, next2_down),
        start(strip(zr, tail), strip(zr, top), below, next2_down, next2_up),
    ]
    densify(cells_n, values_n, dense_y, NSTEP // 2, NSTEP)
    serve_even(1)

    bounds = [None, *(p * PAD for p in PARTS), rows + PAD]
    seen = [False, 2]

    def ready(p):
        need = n_piece if p == len(PARTS) else PARTS[p] + 1
        serve_even(need - len(from_even))
        serve_odd(min(need, n_plain) - len(from_odd))
        if need > n_plain and not seen[0]:
            arrive(*passed_on)
            seen[0] = True

    def ready_far(p):
        need = n_piece if p == len(PARTS) else PARTS[p] + 1
        arrive(*far_odd[seen[1] : need])
        seen[1] = need

    def own_part(p):
        fall(xt, yr, has_next, dense_x, lam_x, own, bounds[p], bounds[p + 1])

    def next_part(p):
        begin_row = -PAD if bounds[p] is None else bounds[p]
        transform(yr, yt.at[0], begin_row, (bounds[p + 1] - begin_row) // PAD)
        rise(yt, bounds[p], bounds[p + 1])

    def next_back(p):
        fall(yt, zr, has_next2, dense_y, lam_y, other, bounds[p], bounds[p + 1])

    n_far = VIA if n_tm > DETOUR else 0
    via, ends, passed = [], [], []

    def send_ends():
        def source(p):
            return xt.at[NSTEP, :, :, pl.ds(p + half_pad, PAD), :]

        for p in pieces[n_piece - n_far :]:
            at = strip(prev_end, p - low)
            via.append(start(source(p), at, (tm + DETOUR, sp), tm == 0, tm == DETOUR))
        for p in pieces[: n_piece - n_far]:
            at = strip(prev_end, p - low)
            ends.append(start(source(p), at, ahead, tm == 0, tm == 1))

    def detour(count):
        for i in range(len(passed), min(len(passed) + count, n_far)):
            arrive(via[i])
            at = strip(prev_end, pieces[n_piece - n_far + i] - low)
            passed.append(start(at, at, back2, tm == DETOUR, tm == 1))

    ready(0)
    arrive(*halo_next)
    own_part(0)
    serve_even(1)
    next_part(0)
    serve_even(n_plain - len(from_even))
    send_ends()
    arrive(*halo_far)
    ready_far(0)
    next_back(0)
    arrive(from_even[0], from_even[1], from_odd[0], from_odd[1])
    halo_carried = [
        start(strip(cr, head), strip(cr, bottom), above, prev2_up, prev2_down),
        start(strip(cr, tail), strip(cr, top), below, prev2_down, prev2_up),
    ]
    ready(1)
    own_part(1)
    detour(1)
    next_part(1)
    detour(1)
    ready_far(1)
    next_back(1)
    detour(n_piece)
    arrive(*from_even[2:], *from_odd[2:], *halo_carried)

    @pl.when(has_prev2)
    def _():
        transform(cr, ct.at[0], -PAD, whole)

        for s in range(NSTEP - 1):
            forward(ct.at[s % 2], ct.at[1 - s % 2], -half_pad, whole - 1, True, True)

    def settle(f, r, before):
        at = at_row(0, r)
        for c in every:
            defect = xr[f, c, at_row(low, r), :] - before(c)
            gradient[f, at, block(c)] = gradient[f, at, block(c)] + defect_weight * defect

    @pl.when(has_prev2)
    def _():
        def one(r):
            out = forward_tile(ct.at[(NSTEP - 1) % 2], r)
            for f in range(3):
                end = raw_end(out[f], f)
                settle(f, r, lambda c, end=end: end[c])

        sweep(0, rows // PAD, one)

    arrive(*ends, *passed)
    for entry in loads[n_early:]:
        entry.wait()

    def plain(before):
        def one(r):
            for f in range(3):
                settle(f, r, lambda c, f=f: before(f, c, at_row(0, r)))

        sweep(0, rows // PAD, one)

    @pl.when(tm == 1)
    def _():
        plain(lambda f, c, at: raw_end(prev_end[f, c, at, :], f))

    @pl.when(tm == 0)
    def _():
        plain(lambda f, c, at: back[f, at, block(c)])

    for entry, sends in started:

        @pl.when(sends)
        def _(entry=entry):
            entry.wait_send()


def solution(mesh):
    n_tm, n_sp = mesh.shape["tm"], mesh.shape["space"]

    def local(states, background, obs_cells, obs_values, land_mask):
        _, fields, rows, cols = states.shape
        padded = rows + 4 * PAD
        lifted = padded + PAD
        blocks = cols // LANES
        block = pltpu.VMEM((fields, rows, cols), jnp.float32)
        f32 = functools.partial(pltpu.VMEM, dtype=jnp.float32)
        i32 = functools.partial(pltpu.VMEM, dtype=jnp.int32)
        n_copy = 16 + 8 * (rows // PAD)
        gradient, nexts = pl.pallas_call(
            functools.partial(kernel, n_tm, n_sp),
            out_shape=(block, block),
            in_specs=[pl.BlockSpec(memory_space=pltpu.HBM)] * 5,
            out_specs=(pl.BlockSpec(memory_space=pltpu.VMEM),) * 2,
            scratch_shapes=[
                f32((fields, blocks, padded, LANES)),
                f32((fields, blocks, padded, LANES)),
                f32((fields, blocks, padded, LANES)),
                f32((fields, blocks, padded, LANES)),
                f32((fields, blocks, rows, LANES)),
                f32((NSTEP + 1, fields, blocks, lifted, LANES)),
                f32((NSTEP + 1, fields, blocks, lifted, LANES)),
                f32((2, fields, blocks, lifted, LANES)),
                f32((NSTEP, fields, blocks, lifted, LANES)),
                f32((NSTEP, fields, blocks, lifted, LANES)),
                i32((blocks, padded, LANES)),
                f32((blocks, lifted, LANES)),
                f32((NSTEP, 2, blocks, rows + PAD, LANES)),
                f32((NSTEP, 2, blocks, rows + PAD, LANES)),
                f32((fields, rows, cols)),
                i32(obs_cells.shape[1:]),
                f32(obs_values.shape[1:]),
                i32(obs_cells.shape[1:]),
                f32(obs_values.shape[1:]),
                pltpu.SemaphoreType.DMA((2 * blocks + 3,)),
                pltpu.SemaphoreType.DMA((n_copy,)),
                pltpu.SemaphoreType.DMA((n_copy,)),
            ],
            compiler_params=pltpu.CompilerParams(
                collective_id=0,
                has_side_effects=True,
                vmem_limit_bytes=56 * 2**20,
            ),
        )(*[
            pltpu.with_memory_space_constraint(x, pltpu.HBM)
            for x in (states[0], background, obs_cells[0], obs_values[0], land_mask)
        ])
        return gradient[None], nexts[None]

    in_specs = (
        P("tm", None, "space", None),
        P(None, "space", None),
        P("tm", None, None),
        P("tm", None, None),
        P("space", None),
    )
    out_specs = (P("tm", None, "space", None), P("tm", None, "space", None))
    return jax.shard_map(local, mesh=mesh, in_specs=in_specs, out_specs=out_specs, check_vma=False)
```

```python
import functools

import jax
import jax.numpy as jnp
from jax import lax
from jax.experimental import pallas as pl
from jax.experimental.pallas import tpu as pltpu
from jax.sharding import PartitionSpec as P

NSTEP = 4
PAD = 8
LANES = 128
DETOUR = 3
UNROLL = 5
LEAD = 2
VIA = 2
PARTS = (4,)

advect = 0.25
gravity = 1.0
coriolis = 0.1
diffuse = 0.1
defect_weight = 2.0
obs_weight = 4.0
step_length = 0.1

KEEP = 1.0 - 4.0 * diffuse
HALF = advect / 2.0
SLOPE = HALF * (advect * gravity / 2.0)

MESH = pl.DeviceIdType.MESH


def kernel(
    n_tm,
    n_sp,
    states,
    background,
    cells_h,
    values_h,
    land,
    gradient,
    nexts,
    xr,
    yr,
    zr,
    cr,
    prev_end,
    xt,
    yt,
    ct,
    lam_x,
    lam_y,
    land_i,
    mask,
    dense_x,
    dense_y,
    back,
    cells,
    values,
    cells_n,
    values_n,
    load,
    send,
    recv,
):
    rows, cols = states.shape[1], states.shape[2]
    blocks = cols // LANES
    tm, sp = lax.axis_index("tm"), lax.axis_index("space")
    low, high = 2 * PAD, 2 * PAD + rows
    half_pad = PAD // 2
    lift = low + half_pad
    has_next, has_next2 = tm < n_tm - 1, tm < n_tm - 2
    has_prev, has_prev2 = tm > 0, tm > 1
    has_up, has_down = sp > 0, sp < n_sp - 1
    every = range(blocks)

    loads = []

    def fetch(src, dst):
        entry = pltpu.make_async_copy(src, dst, load.at[len(loads)])
        entry.start()
        loads.append(entry)

    for c in every:
        part = pl.ds(c * LANES, LANES)
        fetch(states.at[:, :, part], xr.at[:, c, low:high, :])
    n_state = len(loads)
    for c in every:
        part = pl.ds(c * LANES, LANES)
        fetch(land.at[:, part], land_i.at[c, low:high, :])
    fetch(cells_h, cells)
    fetch(values_h, values)
    n_early = len(loads)
    fetch(background, back)

    for at in (PAD, high):
        for ref in (xr, yr, zr, cr):
            ref[:, :, at : at + PAD, :] = jnp.zeros((3, blocks, PAD, LANES), jnp.float32)
        land_i[:, at : at + PAD, :] = jnp.zeros((blocks, PAD, LANES), jnp.int32)

    barrier = pltpu.get_barrier_semaphore()
    near = (
        (has_up, (tm, sp - 1)),
        (has_down, (tm, sp + 1)),
        (has_prev, (tm - 1, sp)),
        (has_next, (tm + 1, sp)),
        (has_prev2, (tm - 2, sp)),
        (has_next2, (tm + 2, sp)),
    )
    if n_tm > DETOUR:
        near += ((tm == 0, (tm + DETOUR, sp)), (tm == DETOUR, (tm - DETOUR, sp)))
    for there, device in near:

        @pl.when(there)
        def _(device=device):
            pl.semaphore_signal(barrier, inc=1, device_id=device, device_id_type=MESH)

    for entry in loads[:n_early]:
        entry.wait()
    pl.semaphore_wait(barrier, sum(there.astype(jnp.int32) for there, _ in near))

    started = []

    def start(src, dst, device, sends, receives):
        index = len(started)
        entry = pltpu.make_async_remote_copy(
            src_ref=src,
            dst_ref=dst,
            send_sem=send.at[index],
            recv_sem=recv.at[index],
            device_id=device,
            device_id_type=MESH,
        )

        @pl.when(sends)
        def _():
            entry.start()

        started.append((entry, sends))
        return entry, receives

    def arrive(*pairs):
        for entry, receives in pairs:

            @pl.when(receives)
            def _(entry=entry):
                entry.wait_recv()

    def strip(ref, at):
        return ref.at[:, :, pl.ds(at, PAD), :]

    above, below = (tm, sp - 1), (tm, sp + 1)
    back1, back2 = (tm - 1, sp), (tm - 2, sp)
    ahead, ahead2 = (tm + 1, sp), (tm + 2, sp)
    top, bottom, head, tail = PAD, high, low, high - PAD

    halo = [
        start(strip(xr, head), strip(xr, bottom), above, has_up, has_down),
        start(strip(xr, tail), strip(xr, top), below, has_down, has_up),
        start(
            land_i.at[:, pl.ds(head, PAD), :],
            land_i.at[:, pl.ds(bottom, PAD), :],
            above,
            has_up,
            has_down,
        ),
        start(
            land_i.at[:, pl.ds(tail, PAD), :],
            land_i.at[:, pl.ds(top, PAD), :],
            below,
            has_down,
            has_up,
        ),
    ]
    even = lax.rem(tm, 2) == 0
    odd = jnp.logical_not(even)
    obs_next = [
        start(cells, cells_n, back1, has_prev, has_next),
        start(values, values_n, back1, has_prev, has_next),
    ]
    pieces = [low, high - PAD, *range(low + PAD, high - PAD, PAD)]
    n_piece = len(pieces)
    n_lead = LEAD
    n_plain = n_piece - n_lead
    odd_prev2, odd_next2 = odd & has_prev2, odd & has_next2
    even_prev2, even_next2 = even & has_prev2, even & has_next2
    lead, passed_on = [], []

    def lead_off(count):
        for p in pieces[n_plain + len(lead) : min(n_plain + len(lead) + count, n_piece)]:
            lead.append(start(strip(xr, p), strip(cr, p), ahead, even_prev2, odd_prev2))

    lead_off(1)
    far_even = [
        start(strip(xr, p), strip(zr, p), back2, even_prev2, even_next2) for p in pieces
    ]
    far_odd = [
        start(strip(xr, p), strip(zr, p), back2, odd_prev2, odd_next2) for p in pieces[:n_plain]
    ]
    direct = [start(strip(xr, p), strip(yr, p), back1, odd, even & has_next) for p in pieces]
    relayed, from_even, from_odd = [], [], []

    def serve_even(count):
        for i in range(len(from_even), min(len(from_even) + count, n_piece)):
            p = pieces[i]
            arrive(far_even[i])
            if i < n_plain:
                relayed.append(
                    start(strip(zr, p), strip(yr, p), ahead, even_next2, odd & has_next)
                )
                lead_off(1)
            arrive(direct[i])
            from_even.append(
                start(strip(yr, p), strip(cr, p), ahead2, even_next2, even_prev2)
            )

    def serve_lead(count):
        for i in range(len(passed_on), min(len(passed_on) + count, n_lead)):
            p = pieces[n_plain + i]
            arrive(lead[i])
            passed_on.append(start(strip(cr, p), strip(yr, p), back2, odd_prev2, odd_next2))
        if len(passed_on) == n_lead:
            for p in pieces[len(far_odd) :]:
                far_odd.append(start(strip(xr, p), strip(zr, p), back2, odd_prev2, odd_next2))

    def serve_odd(count):
        for i in range(len(from_odd), min(len(from_odd) + count, n_plain)):
            p = pieces[i]
            arrive(relayed[i])
            from_odd.append(
                start(strip(yr, p), strip(cr, p), ahead2, odd_next2, odd_prev2)
            )

    first_row = sp * rows - half_pad
    shift = cols.bit_length() - 1
    tall = rows + PAD
    wide = min(2 * LANES, cols)
    wide_shift = wide.bit_length() - 1
    level = lax.broadcasted_iota(jnp.int32, (tall, cells_h.shape[1]), 0)
    column = lax.broadcasted_iota(jnp.int32, (wide, cells_h.shape[1]), 0)

    def densify(cells, values, dense, begin_at, end_at):
        def one(s, carry):
            cell = cells[pl.ds(s, 1), :]
            value = values[pl.ds(s, 1), :]
            row = lax.shift_right_logical(cell, shift) - first_row
            col = lax.bitwise_and(cell, cols - 1)
            inside = (row >= 0) & (row < tall)
            group = lax.shift_right_logical(col, wide_shift)
            key = jnp.where(inside, group * tall + row, -1)
            lane = lax.bitwise_and(col, wide - 1)
            spread = jnp.where(column == lane, 1.0, 0.0).astype(jnp.bfloat16)
            upper = value.astype(jnp.bfloat16).astype(jnp.float32)
            lower = value - upper
            for g in range(cols // wide):
                hit = level == key - g * tall
                picks = jnp.concatenate(
                    [
                        jnp.where(hit, 1.0, 0.0),
                        jnp.where(hit, upper, 0.0),
                        jnp.where(hit, lower, 0.0),
                    ],
                    axis=0,
                ).astype(jnp.bfloat16)
                out = lax.dot_general(
                    picks, spread, (((1,), (1,)), ((), ())), preferred_element_type=jnp.float32
                )
                count = obs_weight * out[:tall]
                total = count + obs_weight * (out[tall : 2 * tall] + out[2 * tall :])
                for c in range(wide // LANES):
                    at = g * (wide // LANES) + c
                    dense[s, 0, at] = count[:, c * LANES : (c + 1) * LANES]
                    dense[s, 1, at] = total[:, c * LANES : (c + 1) * LANES]
            return carry

        lax.fori_loop(begin_at, end_at, one, 0)

    lane_at = lax.broadcasted_iota(jnp.int32, (blocks, PAD, LANES), 2)
    is_first, is_last = lane_at == 0, lane_at == LANES - 1

    def onward(x):
        return jnp.concatenate([x[1:], x[:1]], axis=0)

    def backed(x):
        return jnp.concatenate([x[-1:], x[:-1]], axis=0)

    def from_right(x):
        return pltpu.roll(jnp.where(is_first, onward(x), x), LANES - 1, 2)

    def from_left(x):
        return pltpu.roll(jnp.where(is_last, backed(x), x), 1, 2)

    def turn_right(x):
        turned = pltpu.roll(x, LANES - 1, 2)
        return jnp.where(is_last, onward(turned), turned)

    def turn_left(x):
        turned = pltpu.roll(x, 1, 2)
        return jnp.where(is_first, backed(turned), turned)

    def sweep(first, count, body):
        unroll = max(u for u in range(1, UNROLL + 1) if count % u == 0)

        def group(i, carry):
            for j in range(unroll):
                body(i * (unroll * PAD) + (first + j * PAD))
            return carry

        if count == unroll:
            group(0, 0)
        else:
            lax.fori_loop(0, count // unroll, group, 0)

    def at_row(base, r, lag=0):
        start = r + base
        if (base + lag) % PAD == 0 and not isinstance(start, int):
            start = pl.multiple_of(start, PAD)
        return pl.ds(start, PAD)

    def edges(ref, fill, head_end=True, tail_end=True):
        for there, row, use in ((has_up, -PAD, head_end), (has_down, rows, tail_end)):
            if not use:
                continue

            @pl.when(jnp.logical_not(there))
            def _(row=row):
                for field in range(3):
                    value = jnp.full((blocks, PAD, LANES), fill[field], jnp.float32)
                    ref[field, :, lift + row : lift + row + PAD, :] = value

    def transform(raw, ref, first, count):
        def one(r):
            here, there = at_row(low, r), pl.ds(r + lift, PAD)
            ref[0, :, there, :] = 1.0 + raw[0, :, here, :]
            ref[1, :, there, :] = HALF * raw[1, :, here, :]
            ref[2, :, there, :] = HALF * raw[2, :, here, :]

        sweep(first, count, one)

    def forward_tile(src, r):
        r = r + lift
        here, up, down = pl.ds(r, PAD), pl.ds(r - 1, PAD), pl.ds(r + 1, PAD)
        q, u, v = [src[f, :, here, :] for f in range(3)]
        q_up, q_down = src[0, :, up, :], src[0, :, down, :]
        v_up, v_down = src[2, :, up, :], src[2, :, down, :]
        u_sum = src[1, :, up, :] + src[1, :, down, :]
        m = mask[:, here, :]
        slope, mixed = SLOPE * q, diffuse * u
        q_new = (
            KEEP * q
            + (from_right(q * (diffuse - u)) + from_left(q * (diffuse + u)))
            + (q_up * (diffuse + v_up) + q_down * (diffuse - v_down))
        )
        u_new = m * (
            KEEP * u
            + coriolis * v
            + (from_right(mixed - slope) + from_left(mixed + slope))
            + diffuse * u_sum
        )
        v_new = m * (
            KEEP * v
            - coriolis * u
            + diffuse * ((from_right(v) + from_left(v)) + (v_up + v_down))
            + SLOPE * (q_up - q_down)
        )
        return q_new, u_new, v_new

    def forward(src, dst, first, count, head_end, tail_end):
        def one(r):
            out = forward_tile(src, r)
            here = pl.ds(r + lift, PAD)
            for f in range(3):
                dst[f, :, here, :] = out[f]

        sweep(first, count, one)
        edges(dst, (1.0, 0.0, 0.0), head_end, tail_end)

    def seed(levels, following, there, dense, lam, first, count, head_end, tail_end):
        ends = levels.at[NSTEP]
        weight = jnp.where(there, defect_weight, 0.0)

        def one(r):
            here, raw_at, at = pl.ds(r + lift, PAD), pl.ds(r + low, PAD), drop(r)
            m = mask[:, here, :]
            raw = [jnp.where(there, following[f, :, raw_at, :], 0.0) for f in range(3)]
            pull = weight + dense[NSTEP - 1, 0, :, at, :]
            lam[0, :, here, :] = (
                pull * ends[0, :, here, :]
                - (weight + dense[NSTEP - 1, 1, :, at, :])
                - weight * raw[0]
            )
            for f in (1, 2):
                gap = (weight / (HALF * HALF)) * ends[f, :, here, :]
                lam[f, :, here, :] = m * (gap - (weight / HALF) * raw[f])

        sweep(first, count, one)
        edges(lam, (0.0, 0.0, 0.0), head_end, tail_end)

    def drop(r):
        return pl.ds(r + half_pad, PAD)

    def adjoint_tile(src, state, r):
        r = r + lift
        here, up, down = pl.ds(r, PAD), pl.ds(r - 1, PAD), pl.ds(r + 1, PAD)
        a, b, e = [src[f, :, here, :] for f in range(3)]
        a_right, a_left = turn_right(a), turn_left(a)
        b_right, b_left = turn_right(b), turn_left(b)
        e_right, e_left = turn_right(e), turn_left(e)
        a_up, a_down = src[0, :, up, :], src[0, :, down, :]
        e_up, e_down = src[2, :, up, :], src[2, :, down, :]
        b_sum = src[1, :, up, :] + src[1, :, down, :]
        across, along = a_right - a_left, a_down - a_up
        q = state[0, :, here, :]
        lam_q = (
            KEEP * a
            + diffuse * ((a_right + a_left) + (a_up + a_down))
            + (state[1, :, here, :] * across + state[2, :, here, :] * along)
            + SLOPE * ((b_right - b_left) + (e_down - e_up))
        )
        lam_u = (
            KEEP * b + diffuse * ((b_right + b_left) + b_sum) + q * across - coriolis * e
        )
        lam_v = (
            KEEP * e
            + diffuse * ((e_right + e_left) + (e_up + e_down))
            + q * along
            + coriolis * b
        )
        return lam_q, lam_u, lam_v

    def adjoint(levels, dense, lam, s, first, count, head_end, tail_end):
        src, dst = lam.at[s], lam.at[s - 1]

        def one(r):
            here, at = pl.ds(r + lift, PAD), drop(r)
            out = adjoint_tile(src, levels.at[s], r)
            m = mask[:, here, :]
            push = dense[s - 1, 0, :, at, :] * levels[s, 0, :, here, :]
            dst[0, :, here, :] = out[0] + (push - dense[s - 1, 1, :, at, :])
            dst[1, :, here, :] = m * out[1]
            dst[2, :, here, :] = m * out[2]

        sweep(first, count, one)
        edges(dst, (0.0, 0.0, 0.0), head_end, tail_end)

    def rise(levels, begin_row, end_row):
        upper, lower = begin_row is None, end_row > rows
        begin_row = -PAD if upper else begin_row
        count = (end_row - begin_row) // PAD

        for s in range(NSTEP):
            first = begin_row - 1 - s
            forward(levels.at[s], levels.at[s + 1], first, count, upper, lower)

    def fall(levels, following, there, dense, lam, final, begin_row, end_row):
        upper, lower = begin_row is None, end_row > rows
        begin_row = 0 if upper else begin_row
        count = (end_row - begin_row) // PAD
        first = begin_row - half_pad
        seed(levels, following, there, dense, lam.at[NSTEP - 1], first, count, upper, lower)

        for s in reversed(range(1, NSTEP)):
            lag = 0 if upper else NSTEP - s
            adjoint(levels, dense, lam, s, first - lag, count, upper, lower)

        sweep(
            begin_row if upper else begin_row - PAD,
            count - 1 if upper else count,
            lambda r: final(adjoint_tile(lam.at[0], levels.at[0], r), r),
        )

    def block(c):
        return pl.ds(c * LANES, LANES)

    def raw_end(value, f):
        return value - 1.0 if f == 0 else (1.0 / HALF) * value

    def put(ref, f, at, value):
        for c in every:
            ref[f, at, block(c)] = value[c]

    def own(out, r):
        for f in range(3):
            put(gradient, f, at_row(0, r), out[f] if f == 0 else HALF * out[f])

    def other(out, r):
        here, lifted = at_row(low, r), pl.ds(r + lift, PAD)
        for f in range(3):
            state = yr[f, :, here, :]
            end = raw_end(xt[NSTEP, f, :, lifted, :], f)
            lam = out[f] if f == 0 else HALF * out[f]
            grad = defect_weight * (state - end) + lam
            put(
                nexts, f, at_row(0, r), jnp.where(has_next, state - step_length * grad, end)
            )

    def to_mask(r):
        here, there = at_row(low, r), pl.ds(r + lift, PAD)
        mask[:, there, :] = land_i[:, here, :].astype(jnp.float32)

    whole = (rows + 2 * PAD) // PAD
    densify(cells, values, dense_x, 0, NSTEP)
    serve_even(1)
    serve_lead(1)
    arrive(*halo)
    sweep(-PAD, whole, to_mask)
    transform(xr, xt.at[0], -PAD, whole)

    def own_step(s, carry):
        forward(xt.at[s], xt.at[s + 1], -PAD, whole, True, True)
        return carry

    lax.fori_loop(0, NSTEP // 2, own_step, 0)
    serve_even(1)
    serve_lead(1)
    lax.fori_loop(NSTEP // 2, NSTEP, own_step, 0)
    serve_even(1)
    serve_lead(n_lead)
    arrive(*obs_next)
    densify(cells_n, values_n, dense_y, 0, NSTEP // 2)
    serve_even(1)
    serve_odd(2)
    next_up = has_next & has_up
    next_down = has_next & has_down
    next2_up = has_next2 & has_up
    next2_down = has_next2 & has_down
    prev2_up = has_prev2 & has_up
    prev2_down = has_prev2 & has_down
    halo_next = [
        start(strip(yr, head), strip(yr, bottom), above, next_up, next_down),
        start(strip(yr, tail), strip(yr, top), below, next_down, next_up),
    ]
    arrive(far_odd[0], far_odd[1])
    halo_far = [
        start(strip(zr, head), strip(zr, bottom), above, next2_up, next2_down),
        start(strip(zr, tail), strip(zr, top), below, next2_down, next2_up),
    ]
    densify(cells_n, values_n, dense_y, NSTEP // 2, NSTEP)
    serve_even(1)

    bounds = [None, *(p * PAD for p in PARTS), rows + PAD]
    seen = [False, 2]

    def ready(p):
        need = n_piece if p == len(PARTS) else PARTS[p] + 1
        serve_even(need - len(from_even))
        serve_odd(min(need, n_plain) - len(from_odd))
        if need > n_plain and not seen[0]:
            arrive(*passed_on)
            seen[0] = True

    def ready_far(p):
        need = n_piece if p == len(PARTS) else PARTS[p] + 1
        arrive(*far_odd[seen[1] : need])
        seen[1] = need

    def own_part(p):
        fall(xt, yr, has_next, dense_x, lam_x, own, bounds[p], bounds[p + 1])

    def next_part(p):
        begin_row = -PAD if bounds[p] is None else bounds[p]
        transform(yr, yt.at[0], begin_row, (bounds[p + 1] - begin_row) // PAD)
        rise(yt, bounds[p], bounds[p + 1])

    def next_back(p):
        fall(yt, zr, has_next2, dense_y, lam_y, other, bounds[p], bounds[p + 1])

    n_far = VIA if n_tm > DETOUR else 0
    via, ends, passed = [], [], []

    def send_ends():
        def source(p):
            return xt.at[NSTEP, :, :, pl.ds(p + half_pad, PAD), :]

        for p in pieces[n_piece - n_far :]:
            at = strip(prev_end, p - low)
            via.append(start(source(p), at, (tm + DETOUR, sp), tm == 0, tm == DETOUR))
        for p in pieces[: n_piece - n_far]:
            at = strip(prev_end, p - low)
            ends.append(start(source(p), at, ahead, tm == 0, tm == 1))

    def detour(count):
        for i in range(len(passed), min(len(passed) + count, n_far)):
            arrive(via[i])
            at = strip(prev_end, pieces[n_piece - n_far + i] - low)
            passed.append(start(at, at, back2, tm == DETOUR, tm == 1))

    ready(0)
    arrive(*halo_next)
    own_part(0)
    serve_even(1)
    next_part(0)
    serve_even(n_plain - len(from_even))
    send_ends()
    arrive(*halo_far)
    ready_far(0)
    next_back(0)
    arrive(from_even[0], from_even[1], from_odd[0], from_odd[1])
    halo_carried = [
        start(strip(cr, head), strip(cr, bottom), above, prev2_up, prev2_down),
        start(strip(cr, tail), strip(cr, top), below, prev2_down, prev2_up),
    ]
    ready(1)
    own_part(1)
    detour(1)
    next_part(1)
    detour(1)
    ready_far(1)
    next_back(1)
    detour(n_piece)
    arrive(*from_even[2:], *from_odd[2:], *halo_carried)

    @pl.when(has_prev2)
    def _():
        transform(cr, ct.at[0], -PAD, whole)

        for s in range(NSTEP - 1):
            forward(ct.at[s % 2], ct.at[1 - s % 2], -half_pad, whole - 1, True, True)

    def settle(f, r, before):
        at = at_row(0, r)
        for c in every:
            defect = xr[f, c, at_row(low, r), :] - before(c)
            gradient[f, at, block(c)] = gradient[f, at, block(c)] + defect_weight * defect

    @pl.when(has_prev2)
    def _():
        def one(r):
            out = forward_tile(ct.at[(NSTEP - 1) % 2], r)
            for f in range(3):
                end = raw_end(out[f], f)
                settle(f, r, lambda c, end=end: end[c])

        sweep(0, rows // PAD, one)

    for entry in loads[n_early:]:
        entry.wait()

    def plain(before):
        def one(r):
            for f in range(3):
                settle(f, r, lambda c, f=f: before(f, c, at_row(0, r)))

        sweep(0, rows // PAD, one)

    @pl.when(tm == 1)
    def _():
        for pair, p in zip(ends + passed, pieces):
            pair[0].wait_recv()
            at = at_row(0, p - low)
            for f in range(3):
                end = raw_end(prev_end[f, :, at, :], f)
                settle(f, p - low, lambda c, end=end: end[c])

    @pl.when(tm == 0)
    def _():
        plain(lambda f, c, at: back[f, at, block(c)])

    for entry, sends in started:

        @pl.when(sends)
        def _(entry=entry):
            entry.wait_send()


def solution(mesh):
    n_tm, n_sp = mesh.shape["tm"], mesh.shape["space"]

    def local(states, background, obs_cells, obs_values, land_mask):
        _, fields, rows, cols = states.shape
        padded = rows + 4 * PAD
        lifted = padded + PAD
        blocks = cols // LANES
        block = pltpu.VMEM((fields, rows, cols), jnp.float32)
        f32 = functools.partial(pltpu.VMEM, dtype=jnp.float32)
        i32 = functools.partial(pltpu.VMEM, dtype=jnp.int32)
        n_copy = 16 + 8 * (rows // PAD)
        gradient, nexts = pl.pallas_call(
            functools.partial(kernel, n_tm, n_sp),
            out_shape=(block, block),
            in_specs=[pl.BlockSpec(memory_space=pltpu.HBM)] * 5,
            out_specs=(pl.BlockSpec(memory_space=pltpu.VMEM),) * 2,
            scratch_shapes=[
                f32((fields, blocks, padded, LANES)),
                f32((fields, blocks, padded, LANES)),
                f32((fields, blocks, padded, LANES)),
                f32((fields, blocks, padded, LANES)),
                f32((fields, blocks, rows, LANES)),
                f32((NSTEP + 1, fields, blocks, lifted, LANES)),
                f32((NSTEP + 1, fields, blocks, lifted, LANES)),
                f32((2, fields, blocks, lifted, LANES)),
                f32((NSTEP, fields, blocks, lifted, LANES)),
                f32((NSTEP, fields, blocks, lifted, LANES)),
                i32((blocks, padded, LANES)),
                f32((blocks, lifted, LANES)),
                f32((NSTEP, 2, blocks, rows + PAD, LANES)),
                f32((NSTEP, 2, blocks, rows + PAD, LANES)),
                f32((fields, rows, cols)),
                i32(obs_cells.shape[1:]),
                f32(obs_values.shape[1:]),
                i32(obs_cells.shape[1:]),
                f32(obs_values.shape[1:]),
                pltpu.SemaphoreType.DMA((2 * blocks + 3,)),
                pltpu.SemaphoreType.DMA((n_copy,)),
                pltpu.SemaphoreType.DMA((n_copy,)),
            ],
            compiler_params=pltpu.CompilerParams(
                collective_id=0,
                has_side_effects=True,
                vmem_limit_bytes=56 * 2**20,
            ),
        )(*[
            pltpu.with_memory_space_constraint(x, pltpu.HBM)
            for x in (states[0], background, obs_cells[0], obs_values[0], land_mask)
        ])
        return gradient[None], nexts[None]

    in_specs = (
        P("tm", None, "space", None),
        P(None, "space", None),
        P("tm", None, None),
        P("tm", None, None),
        P("space", None),
    )
    out_specs = (P("tm", None, "space", None), P("tm", None, "space", None))
    return jax.shard_map(local, mesh=mesh, in_specs=in_specs, out_specs=out_specs, check_vma=False)
```

```python
import functools

import jax
import jax.numpy as jnp
from jax import lax
from jax.experimental import pallas as pl
from jax.experimental.pallas import tpu as pltpu
from jax.sharding import PartitionSpec as P

NSTEP = 4
PAD = 8
LANES = 128
DETOUR = 3
UNROLL = 5
LEAD = 2
AHEAD = 3
VIA = 2
PARTS = (4,)

advect = 0.25
gravity = 1.0
coriolis = 0.1
diffuse = 0.1
defect_weight = 2.0
obs_weight = 4.0
step_length = 0.1

KEEP = 1.0 - 4.0 * diffuse
HALF = advect / 2.0
SLOPE = HALF * (advect * gravity / 2.0)

MESH = pl.DeviceIdType.MESH


def kernel(
    n_tm,
    n_sp,
    states,
    background,
    cells_h,
    values_h,
    land,
    gradient,
    nexts,
    xr,
    yr,
    zr,
    cr,
    prev_end,
    xt,
    yt,
    ct,
    lam_x,
    lam_y,
    land_i,
    mask,
    dense_x,
    dense_y,
    back,
    cells,
    values,
    cells_n,
    values_n,
    load,
    send,
    recv,
):
    rows, cols = states.shape[1], states.shape[2]
    blocks = cols // LANES
    tm, sp = lax.axis_index("tm"), lax.axis_index("space")
    low, high = 2 * PAD, 2 * PAD + rows
    half_pad = PAD // 2
    lift = low + half_pad
    has_next, has_next2 = tm < n_tm - 1, tm < n_tm - 2
    has_prev, has_prev2 = tm > 0, tm > 1
    has_up, has_down = sp > 0, sp < n_sp - 1
    every = range(blocks)

    loads = []

    def fetch(src, dst):
        entry = pltpu.make_async_copy(src, dst, load.at[len(loads)])
        entry.start()
        loads.append(entry)

    for c in every:
        part = pl.ds(c * LANES, LANES)
        fetch(states.at[:, :, part], xr.at[:, c, low:high, :])
    n_state = len(loads)
    for c in every:
        part = pl.ds(c * LANES, LANES)
        fetch(land.at[:, part], land_i.at[c, low:high, :])
    fetch(cells_h, cells)
    fetch(values_h, values)
    n_early = len(loads)
    fetch(background, back)

    for at in (PAD, high):
        for ref in (xr, yr, zr, cr):
            ref[:, :, at : at + PAD, :] = jnp.zeros((3, blocks, PAD, LANES), jnp.float32)
        land_i[:, at : at + PAD, :] = jnp.zeros((blocks, PAD, LANES), jnp.int32)

    barrier = pltpu.get_barrier_semaphore()
    near = (
        (has_up, (tm, sp - 1)),
        (has_down, (tm, sp + 1)),
        (has_prev, (tm - 1, sp)),
        (has_next, (tm + 1, sp)),
        (has_prev2, (tm - 2, sp)),
        (has_next2, (tm + 2, sp)),
    )
    if n_tm > DETOUR:
        near += ((tm == 0, (tm + DETOUR, sp)), (tm == DETOUR, (tm - DETOUR, sp)))
    for there, device in near:

        @pl.when(there)
        def _(device=device):
            pl.semaphore_signal(barrier, inc=1, device_id=device, device_id_type=MESH)

    for entry in loads[:n_early]:
        entry.wait()
    pl.semaphore_wait(barrier, sum(there.astype(jnp.int32) for there, _ in near))

    started = []

    def start(src, dst, device, sends, receives):
        index = len(started)
        entry = pltpu.make_async_remote_copy(
            src_ref=src,
            dst_ref=dst,
            send_sem=send.at[index],
            recv_sem=recv.at[index],
            device_id=device,
            device_id_type=MESH,
        )

        @pl.when(sends)
        def _():
            entry.start()

        started.append((entry, sends))
        return entry, receives

    def arrive(*pairs):
        for entry, receives in pairs:

            @pl.when(receives)
            def _(entry=entry):
                entry.wait_recv()

    def strip(ref, at):
        return ref.at[:, :, pl.ds(at, PAD), :]

    above, below = (tm, sp - 1), (tm, sp + 1)
    back1, back2 = (tm - 1, sp), (tm - 2, sp)
    ahead, ahead2 = (tm + 1, sp), (tm + 2, sp)
    top, bottom, head, tail = PAD, high, low, high - PAD

    halo = [
        start(strip(xr, head), strip(xr, bottom), above, has_up, has_down),
        start(strip(xr, tail), strip(xr, top), below, has_down, has_up),
        start(
            land_i.at[:, pl.ds(head, PAD), :],
            land_i.at[:, pl.ds(bottom, PAD), :],
            above,
            has_up,
            has_down,
        ),
        start(
            land_i.at[:, pl.ds(tail, PAD), :],
            land_i.at[:, pl.ds(top, PAD), :],
            below,
            has_down,
            has_up,
        ),
    ]
    even = lax.rem(tm, 2) == 0
    odd = jnp.logical_not(even)
    obs_next = [
        start(cells, cells_n, back1, has_prev, has_next),
        start(values, values_n, back1, has_prev, has_next),
    ]
    pieces = [low, high - PAD, *range(low + PAD, high - PAD, PAD)]
    n_piece = len(pieces)
    n_lead = LEAD
    n_plain = n_piece - n_lead
    odd_prev2, odd_next2 = odd & has_prev2, odd & has_next2
    even_prev2, even_next2 = even & has_prev2, even & has_next2
    lead, passed_on = [], []

    def lead_off(count):
        for p in pieces[n_plain + len(lead) : min(n_plain + len(lead) + count, n_piece)]:
            lead.append(start(strip(xr, p), strip(cr, p), ahead, even_prev2, odd_prev2))

    lead_off(1)
    far_even, far_odd, direct = [], {}, []

    def push(count):
        for i in range(len(direct), min(len(direct) + count, n_piece)):
            p = pieces[i]
            far_even.append(
                start(strip(xr, p), strip(zr, p), back2, even_prev2, even_next2)
            )
            direct.append(start(strip(xr, p), strip(yr, p), back1, odd, even & has_next))
            if i < n_plain:
                far_odd[i] = start(strip(xr, p), strip(zr, p), back2, odd_prev2, odd_next2)

    push(AHEAD)
    relayed, from_even, from_odd = [], [], []

    def serve_even(count):
        for i in range(len(from_even), min(len(from_even) + count, n_piece)):
            p = pieces[i]
            push(1)
            arrive(far_even[i])
            if i < n_plain:
                relayed.append(
                    start(strip(zr, p), strip(yr, p), ahead, even_next2, odd & has_next)
                )
                lead_off(1)
            arrive(direct[i])
            from_even.append(
                start(strip(yr, p), strip(cr, p), ahead2, even_next2, even_prev2)
            )

    def serve_lead(count):
        for i in range(len(passed_on), min(len(passed_on) + count, n_lead)):
            p = pieces[n_plain + i]
            arrive(lead[i])
            passed_on.append(start(strip(cr, p), strip(yr, p), back2, odd_prev2, odd_next2))
        if len(passed_on) == n_lead and n_plain not in far_odd:
            for i, p in list(enumerate(pieces))[n_plain:]:
                far_odd[i] = start(strip(xr, p), strip(zr, p), back2, odd_prev2, odd_next2)

    def serve_odd(count):
        for i in range(len(from_odd), min(len(from_odd) + count, n_plain)):
            p = pieces[i]
            arrive(relayed[i])
            from_odd.append(
                start(strip(yr, p), strip(cr, p), ahead2, odd_next2, odd_prev2)
            )

    first_row = sp * rows - half_pad
    shift = cols.bit_length() - 1
    tall = rows + PAD
    wide = min(2 * LANES, cols)
    wide_shift = wide.bit_length() - 1
    level = lax.broadcasted_iota(jnp.int32, (tall, cells_h.shape[1]), 0)
    column = lax.broadcasted_iota(jnp.int32, (wide, cells_h.shape[1]), 0)

    def densify(cells, values, dense, begin_at, end_at):
        def one(s, carry):
            cell = cells[pl.ds(s, 1), :]
            value = values[pl.ds(s, 1), :]
            row = lax.shift_right_logical(cell, shift) - first_row
            col = lax.bitwise_and(cell, cols - 1)
            inside = (row >= 0) & (row < tall)
            group = lax.shift_right_logical(col, wide_shift)
            key = jnp.where(inside, group * tall + row, -1)
            lane = lax.bitwise_and(col, wide - 1)
            spread = jnp.where(column == lane, 1.0, 0.0).astype(jnp.bfloat16)
            upper = value.astype(jnp.bfloat16).astype(jnp.float32)
            lower = value - upper
            for g in range(cols // wide):
                hit = level == key - g * tall
                picks = jnp.concatenate(
                    [
                        jnp.where(hit, 1.0, 0.0),
                        jnp.where(hit, upper, 0.0),
                        jnp.where(hit, lower, 0.0),
                    ],
                    axis=0,
                ).astype(jnp.bfloat16)
                out = lax.dot_general(
                    picks, spread, (((1,), (1,)), ((), ())), preferred_element_type=jnp.float32
                )
                count = obs_weight * out[:tall]
                total = count + obs_weight * (out[tall : 2 * tall] + out[2 * tall :])
                for c in range(wide // LANES):
                    at = g * (wide // LANES) + c
                    dense[s, 0, at] = count[:, c * LANES : (c + 1) * LANES]
                    dense[s, 1, at] = total[:, c * LANES : (c + 1) * LANES]
            return carry

        lax.fori_loop(begin_at, end_at, one, 0)

    lane_at = lax.broadcasted_iota(jnp.int32, (blocks, PAD, LANES), 2)
    is_first, is_last = lane_at == 0, lane_at == LANES - 1

    def onward(x):
        return jnp.concatenate([x[1:], x[:1]], axis=0)

    def backed(x):
        return jnp.concatenate([x[-1:], x[:-1]], axis=0)

    def from_right(x):
        return pltpu.roll(jnp.where(is_first, onward(x), x), LANES - 1, 2)

    def from_left(x):
        return pltpu.roll(jnp.where(is_last, backed(x), x), 1, 2)

    def turn_right(x):
        turned = pltpu.roll(x, LANES - 1, 2)
        return jnp.where(is_last, onward(turned), turned)

    def turn_left(x):
        turned = pltpu.roll(x, 1, 2)
        return jnp.where(is_first, backed(turned), turned)

    def sweep(first, count, body):
        unroll = max(u for u in range(1, UNROLL + 1) if count % u == 0)

        def group(i, carry):
            for j in range(unroll):
                body(i * (unroll * PAD) + (first + j * PAD))
            return carry

        if count == unroll:
            group(0, 0)
        else:
            lax.fori_loop(0, count // unroll, group, 0)

    def at_row(base, r, lag=0):
        start = r + base
        if (base + lag) % PAD == 0 and not isinstance(start, int):
            start = pl.multiple_of(start, PAD)
        return pl.ds(start, PAD)

    def edges(ref, fill, head_end=True, tail_end=True):
        for there, row, use in ((has_up, -PAD, head_end), (has_down, rows, tail_end)):
            if not use:
                continue

            @pl.when(jnp.logical_not(there))
            def _(row=row):
                for field in range(3):
                    value = jnp.full((blocks, PAD, LANES), fill[field], jnp.float32)
                    ref[field, :, lift + row : lift + row + PAD, :] = value

    def transform(raw, ref, first, count):
        def one(r):
            here, there = at_row(low, r), pl.ds(r + lift, PAD)
            ref[0, :, there, :] = 1.0 + raw[0, :, here, :]
            ref[1, :, there, :] = HALF * raw[1, :, here, :]
            ref[2, :, there, :] = HALF * raw[2, :, here, :]

        sweep(first, count, one)

    def forward_tile(src, r):
        r = r + lift
        here, up, down = pl.ds(r, PAD), pl.ds(r - 1, PAD), pl.ds(r + 1, PAD)
        q, u, v = [src[f, :, here, :] for f in range(3)]
        q_up, q_down = src[0, :, up, :], src[0, :, down, :]
        v_up, v_down = src[2, :, up, :], src[2, :, down, :]
        u_sum = src[1, :, up, :] + src[1, :, down, :]
        m = mask[:, here, :]
        slope, mixed = SLOPE * q, diffuse * u
        q_new = (
            KEEP * q
            + (from_right(q * (diffuse - u)) + from_left(q * (diffuse + u)))
            + (q_up * (diffuse + v_up) + q_down * (diffuse - v_down))
        )
        u_new = m * (
            KEEP * u
            + coriolis * v
            + (from_right(mixed - slope) + from_left(mixed + slope))
            + diffuse * u_sum
        )
        v_new = m * (
            KEEP * v
            - coriolis * u
            + diffuse * ((from_right(v) + from_left(v)) + (v_up + v_down))
            + SLOPE * (q_up - q_down)
        )
        return q_new, u_new, v_new

    def forward(src, dst, first, count, head_end, tail_end):
        def one(r):
            out = forward_tile(src, r)
            here = pl.ds(r + lift, PAD)
            for f in range(3):
                dst[f, :, here, :] = out[f]

        sweep(first, count, one)
        edges(dst, (1.0, 0.0, 0.0), head_end, tail_end)

    def seed(levels, following, there, dense, lam, first, count, head_end, tail_end):
        ends = levels.at[NSTEP]
        weight = jnp.where(there, defect_weight, 0.0)

        def one(r):
            here, raw_at, at = pl.ds(r + lift, PAD), pl.ds(r + low, PAD), drop(r)
            m = mask[:, here, :]
            raw = [jnp.where(there, following[f, :, raw_at, :], 0.0) for f in range(3)]
            pull = weight + dense[NSTEP - 1, 0, :, at, :]
            lam[0, :, here, :] = (
                pull * ends[0, :, here, :]
                - (weight + dense[NSTEP - 1, 1, :, at, :])
                - weight * raw[0]
            )
            for f in (1, 2):
                gap = (weight / (HALF * HALF)) * ends[f, :, here, :]
                lam[f, :, here, :] = m * (gap - (weight / HALF) * raw[f])

        sweep(first, count, one)
        edges(lam, (0.0, 0.0, 0.0), head_end, tail_end)

    def drop(r):
        return pl.ds(r + half_pad, PAD)

    def adjoint_tile(src, state, r):
        r = r + lift
        here, up, down = pl.ds(r, PAD), pl.ds(r - 1, PAD), pl.ds(r + 1, PAD)
        a, b, e = [src[f, :, here, :] for f in range(3)]
        a_right, a_left = turn_right(a), turn_left(a)
        b_right, b_left = turn_right(b), turn_left(b)
        e_right, e_left = turn_right(e), turn_left(e)
        a_up, a_down = src[0, :, up, :], src[0, :, down, :]
        e_up, e_down = src[2, :, up, :], src[2, :, down, :]
        b_sum = src[1, :, up, :] + src[1, :, down, :]
        across, along = a_right - a_left, a_down - a_up
        q = state[0, :, here, :]
        lam_q = (
            KEEP * a
            + diffuse * ((a_right + a_left) + (a_up + a_down))
            + (state[1, :, here, :] * across + state[2, :, here, :] * along)
            + SLOPE * ((b_right - b_left) + (e_down - e_up))
        )
        lam_u = (
            KEEP * b + diffuse * ((b_right + b_left) + b_sum) + q * across - coriolis * e
        )
        lam_v = (
            KEEP * e
            + diffuse * ((e_right + e_left) + (e_up + e_down))
            + q * along
            + coriolis * b
        )
        return lam_q, lam_u, lam_v

    def adjoint(levels, dense, lam, s, first, count, head_end, tail_end):
        src, dst = lam.at[s], lam.at[s - 1]

        def one(r):
            here, at = pl.ds(r + lift, PAD), drop(r)
            out = adjoint_tile(src, levels.at[s], r)
            m = mask[:, here, :]
            push = dense[s - 1, 0, :, at, :] * levels[s, 0, :, here, :]
            dst[0, :, here, :] = out[0] + (push - dense[s - 1, 1, :, at, :])
            dst[1, :, here, :] = m * out[1]
            dst[2, :, here, :] = m * out[2]

        sweep(first, count, one)
        edges(dst, (0.0, 0.0, 0.0), head_end, tail_end)

    def rise(levels, begin_row, end_row):
        upper, lower = begin_row is None, end_row > rows
        begin_row = -PAD if upper else begin_row
        count = (end_row - begin_row) // PAD

        for s in range(NSTEP):
            first = begin_row - 1 - s
            forward(levels.at[s], levels.at[s + 1], first, count, upper, lower)

    def fall(levels, following, there, dense, lam, final, begin_row, end_row):
        upper, lower = begin_row is None, end_row > rows
        begin_row = 0 if upper else begin_row
        count = (end_row - begin_row) // PAD
        first = begin_row - half_pad
        seed(levels, following, there, dense, lam.at[NSTEP - 1], first, count, upper, lower)

        for s in reversed(range(1, NSTEP)):
            lag = 0 if upper else NSTEP - s
            adjoint(levels, dense, lam, s, first - lag, count, upper, lower)

        sweep(
            begin_row if upper else begin_row - PAD,
            count - 1 if upper else count,
            lambda r: final(adjoint_tile(lam.at[0], levels.at[0], r), r),
        )

    def block(c):
        return pl.ds(c * LANES, LANES)

    def raw_end(value, f):
        return value - 1.0 if f == 0 else (1.0 / HALF) * value

    def put(ref, f, at, value):
        for c in every:
            ref[f, at, block(c)] = value[c]

    def own(out, r):
        for f in range(3):
            put(gradient, f, at_row(0, r), out[f] if f == 0 else HALF * out[f])

    def other(out, r):
        here, lifted = at_row(low, r), pl.ds(r + lift, PAD)
        for f in range(3):
            state = yr[f, :, here, :]
            end = raw_end(xt[NSTEP, f, :, lifted, :], f)
            lam = out[f] if f == 0 else HALF * out[f]
            grad = defect_weight * (state - end) + lam
            put(
                nexts, f, at_row(0, r), jnp.where(has_next, state - step_length * grad, end)
            )

    def to_mask(r):
        here, there = at_row(low, r), pl.ds(r + lift, PAD)
        mask[:, there, :] = land_i[:, here, :].astype(jnp.float32)

    whole = (rows + 2 * PAD) // PAD
    densify(cells, values, dense_x, 0, NSTEP)
    serve_even(1)
    serve_lead(1)
    arrive(*halo)
    sweep(-PAD, whole, to_mask)
    transform(xr, xt.at[0], -PAD, whole)

    def own_step(s, carry):
        forward(xt.at[s], xt.at[s + 1], -PAD, whole, True, True)
        return carry

    lax.fori_loop(0, NSTEP // 2, own_step, 0)
    serve_even(1)
    serve_lead(1)
    lax.fori_loop(NSTEP // 2, NSTEP, own_step, 0)
    serve_even(1)
    serve_lead(n_lead)
    arrive(*obs_next)
    densify(cells_n, values_n, dense_y, 0, NSTEP // 2)
    serve_even(1)
    serve_odd(2)
    next_up = has_next & has_up
    next_down = has_next & has_down
    next2_up = has_next2 & has_up
    next2_down = has_next2 & has_down
    prev2_up = has_prev2 & has_up
    prev2_down = has_prev2 & has_down
    halo_next = [
        start(strip(yr, head), strip(yr, bottom), above, next_up, next_down),
        start(strip(yr, tail), strip(yr, top), below, next_down, next_up),
    ]
    arrive(far_odd[0], far_odd[1])
    halo_far = [
        start(strip(zr, head), strip(zr, bottom), above, next2_up, next2_down),
        start(strip(zr, tail), strip(zr, top), below, next2_down, next2_up),
    ]
    densify(cells_n, values_n, dense_y, NSTEP // 2, NSTEP)
    serve_even(1)

    bounds = [None, *(p * PAD for p in PARTS), rows + PAD]
    seen = [False, 2]

    def ready(p):
        need = n_piece if p == len(PARTS) else PARTS[p] + 1
        serve_even(need - len(from_even))
        serve_odd(min(need, n_plain) - len(from_odd))
        if need > n_plain and not seen[0]:
            arrive(*passed_on)
            seen[0] = True

    def ready_far(p):
        need = n_piece if p == len(PARTS) else PARTS[p] + 1
        arrive(*(far_odd[i] for i in range(seen[1], need)))
        seen[1] = need

    def own_part(p):
        fall(xt, yr, has_next, dense_x, lam_x, own, bounds[p], bounds[p + 1])

    def next_part(p):
        begin_row = -PAD if bounds[p] is None else bounds[p]
        transform(yr, yt.at[0], begin_row, (bounds[p + 1] - begin_row) // PAD)
        rise(yt, bounds[p], bounds[p + 1])

    def next_back(p):
        fall(yt, zr, has_next2, dense_y, lam_y, other, bounds[p], bounds[p + 1])

    n_far = VIA if n_tm > DETOUR else 0
    via, ends, passed = [], [], []

    def send_ends():
        def source(p):
            return xt.at[NSTEP, :, :, pl.ds(p + half_pad, PAD), :]

        for p in pieces[n_piece - n_far :]:
            at = strip(prev_end, p - low)
            via.append(start(source(p), at, (tm + DETOUR, sp), tm == 0, tm == DETOUR))
        for p in pieces[: n_piece - n_far]:
            at = strip(prev_end, p - low)
            ends.append(start(source(p), at, ahead, tm == 0, tm == 1))

    def detour(count):
        for i in range(len(passed), min(len(passed) + count, n_far)):
            arrive(via[i])
            at = strip(prev_end, pieces[n_piece - n_far + i] - low)
            passed.append(start(at, at, back2, tm == DETOUR, tm == 1))

    ready(0)
    arrive(*halo_next)
    own_part(0)
    serve_even(1)
    next_part(0)
    serve_even(n_plain - len(from_even))
    send_ends()
    arrive(*halo_far)
    ready_far(0)
    next_back(0)
    arrive(from_even[0], from_even[1], from_odd[0], from_odd[1])
    halo_carried = [
        start(strip(cr, head), strip(cr, bottom), above, prev2_up, prev2_down),
        start(strip(cr, tail), strip(cr, top), below, prev2_down, prev2_up),
    ]
    ready(1)
    own_part(1)
    detour(1)
    next_part(1)
    detour(1)
    ready_far(1)
    next_back(1)
    detour(n_piece)
    arrive(*from_even[2:], *from_odd[2:], *halo_carried)

    @pl.when(has_prev2)
    def _():
        transform(cr, ct.at[0], -PAD, whole)

        for s in range(NSTEP - 1):
            forward(ct.at[s % 2], ct.at[1 - s % 2], -half_pad, whole - 1, True, True)

    def settle(f, r, before):
        at = at_row(0, r)
        for c in every:
            defect = xr[f, c, at_row(low, r), :] - before(c)
            gradient[f, at, block(c)] = gradient[f, at, block(c)] + defect_weight * defect

    @pl.when(has_prev2)
    def _():
        def one(r):
            out = forward_tile(ct.at[(NSTEP - 1) % 2], r)
            for f in range(3):
                end = raw_end(out[f], f)
                settle(f, r, lambda c, end=end: end[c])

        sweep(0, rows // PAD, one)

    for entry in loads[n_early:]:
        entry.wait()

    def plain(before):
        def one(r):
            for f in range(3):
                settle(f, r, lambda c, f=f: before(f, c, at_row(0, r)))

        sweep(0, rows // PAD, one)

    @pl.when(tm == 1)
    def _():
        for pair, p in zip(ends + passed, pieces):
            pair[0].wait_recv()
            at = at_row(0, p - low)
            for f in range(3):
                end = raw_end(prev_end[f, :, at, :], f)
                settle(f, p - low, lambda c, end=end: end[c])

    @pl.when(tm == 0)
    def _():
        plain(lambda f, c, at: back[f, at, block(c)])

    for entry, sends in started:

        @pl.when(sends)
        def _(entry=entry):
            entry.wait_send()


def solution(mesh):
    n_tm, n_sp = mesh.shape["tm"], mesh.shape["space"]

    def local(states, background, obs_cells, obs_values, land_mask):
        _, fields, rows, cols = states.shape
        padded = rows + 4 * PAD
        lifted = padded + PAD
        blocks = cols // LANES
        block = pltpu.VMEM((fields, rows, cols), jnp.float32)
        f32 = functools.partial(pltpu.VMEM, dtype=jnp.float32)
        i32 = functools.partial(pltpu.VMEM, dtype=jnp.int32)
        n_copy = 16 + 8 * (rows // PAD)
        gradient, nexts = pl.pallas_call(
            functools.partial(kernel, n_tm, n_sp),
            out_shape=(block, block),
            in_specs=[pl.BlockSpec(memory_space=pltpu.HBM)] * 5,
            out_specs=(pl.BlockSpec(memory_space=pltpu.VMEM),) * 2,
            scratch_shapes=[
                f32((fields, blocks, padded, LANES)),
                f32((fields, blocks, padded, LANES)),
                f32((fields, blocks, padded, LANES)),
                f32((fields, blocks, padded, LANES)),
                f32((fields, blocks, rows, LANES)),
                f32((NSTEP + 1, fields, blocks, lifted, LANES)),
                f32((NSTEP + 1, fields, blocks, lifted, LANES)),
                f32((2, fields, blocks, lifted, LANES)),
                f32((NSTEP, fields, blocks, lifted, LANES)),
                f32((NSTEP, fields, blocks, lifted, LANES)),
                i32((blocks, padded, LANES)),
                f32((blocks, lifted, LANES)),
                f32((NSTEP, 2, blocks, rows + PAD, LANES)),
                f32((NSTEP, 2, blocks, rows + PAD, LANES)),
                f32((fields, rows, cols)),
                i32(obs_cells.shape[1:]),
                f32(obs_values.shape[1:]),
                i32(obs_cells.shape[1:]),
                f32(obs_values.shape[1:]),
                pltpu.SemaphoreType.DMA((2 * blocks + 3,)),
                pltpu.SemaphoreType.DMA((n_copy,)),
                pltpu.SemaphoreType.DMA((n_copy,)),
            ],
            compiler_params=pltpu.CompilerParams(
                collective_id=0,
                has_side_effects=True,
                vmem_limit_bytes=56 * 2**20,
            ),
        )(*[
            pltpu.with_memory_space_constraint(x, pltpu.HBM)
            for x in (states[0], background, obs_cells[0], obs_values[0], land_mask)
        ])
        return gradient[None], nexts[None]

    in_specs = (
        P("tm", None, "space", None),
        P(None, "space", None),
        P("tm", None, None),
        P("tm", None, None),
        P("space", None),
    )
    out_specs = (P("tm", None, "space", None), P("tm", None, "space", None))
    return jax.shard_map(local, mesh=mesh, in_specs=in_specs, out_specs=out_specs, check_vma=False)
```
